32 devices in a mesh: role: 2 (over x), dp: 4 (over y, core), ctx: 4 (over z).
Axes of the slice: x: 2, y: 2, z: 4, core: 2. Of those that a mesh axis runs over, the one named last changes fastest.
Arguments:
- teacher_states: bfloat16 [4, 512, 5120], P('dp', 'ctx'), may hold values from -50 to 50
- student_states: bfloat16 [4, 512, 3584], P('dp', 'ctx'), may hold values from -50 to 50
- teacher_gain: float32 [5120], replicated, may hold values from 0.25 to 1.75
- student_gain: float32 [3584], replicated, may hold values from 0.25 to 1.75
- mentor_output_weights: bfloat16 [4, 5120, 2048], P(None, None, 'ctx'), may hold values from -2 to 2
- student_heads: bfloat16 [4, 3584, 2048], P(None, None, 'ctx'), may hold values from -2 to 2
- segments: int32 [4, 512], P('dp', 'ctx'), may hold values from 0 to 7, never falling along the last dimension, each value on 1 to 256 neighbouring positions
- targets: int32 [4, 512, 4], P('dp', 'ctx'), may hold values from 0 to 2047
Outputs:
- grad_heads: float32 [4, 3584, 2048], P(None, ('role', 'dp'), 'ctx')
- frame_terms: float32 [2, 4, 512, 4], P('role', 'dp', 'ctx')
The draws below stay inside these ranges and needn't reach their ends.
All inputs are finite; a program needn't handle non-finite values.
Results may differ from the reference program's by a relative error of at most 0.0048.
Values may be sent and summed in bfloat16 or wider, within the bound.
A program may use at most 192 MiB of HBM per device.

```python
import math
import jax
import jax.numpy as jnp
import numpy as np
from jax import lax

DT = 5120
DS = 3584
CODE_ALPHABET = 2048
QUANTIZER_TOTAL = 4
ROW_DEV = 128
SEQUENCE_STEPS = 512
DOCS = 8
N_DP = 4


def states_draw(key, seed_tag, model_width):
    values = jnp.clip(jax.random.normal(jax.random.fold_in(key, seed_tag), (N_DP, SEQUENCE_STEPS, model_width), jnp.float32), -5.0, 5.0)
    return values.astype(jnp.bfloat16)


def heads_draw(key, seed_tag, model_width):
    values = jnp.clip(jax.random.normal(jax.random.fold_in(key, seed_tag), (QUANTIZER_TOTAL, model_width, CODE_ALPHABET), jnp.float32), -5.0, 5.0)
    values = values * (3.0 / math.sqrt(model_width))
    return values.astype(jnp.bfloat16)


def draw_teacher_states(key, part):
    return states_draw(key, 11, DT)


def draw_student_states(key, part):
    return states_draw(key, 21, DS)


def draw_mentor_output_weights(key, part):
    return heads_draw(key, 31, DT)


def draw_student_heads(key, part):
    return heads_draw(key, 41, DS)


def place_ends(drawn, stream_key, low, top_value):
    index_at = [jax.random.randint(jax.random.fold_in(stream_key, axis), (), 0, length) for axis, length in enumerate(drawn.shape)]
    widest = drawn.shape.index(max(drawn.shape))
    neighbour = index_at[:widest] + [(index_at[widest] + 1) % drawn.shape[widest]] + index_at[widest + 1:]
    return drawn.at[tuple(index_at)].set(low).at[tuple(neighbour)].set(top_value)


def length_profile(number_of, total, limit, skew):
    weights = [(1 << 20) // math.isqrt(grade ** skew) + 1 for grade in range(2, number_of + 1)]
    rest, holding = total - limit - (number_of - 1), [1] * (number_of - 1)
    while rest > 0:
        free = [i for i in range(number_of - 1) if holding[i] < limit]
        mass, remaining = sum([weights[i] for i in free]), rest
        for i in free:
            addition = min(limit - holding[i], max(1, remaining * weights[i] // mass), rest)
            holding[i] = holding[i] + addition
            rest = rest - addition
    return np.array([limit] + holding)


def ragged(own_key, number_of, total, bound, skew):
    if number_of == 2:
        one = jax.random.randint(own_key, (), max(1, total - bound), min(bound, total - 1) + 1)
        return jnp.stack([one, total - one])
    sizes = jnp.asarray(length_profile(number_of, total, bound, skew), jnp.int32)
    twos = (number_of - 1) // 2
    source_of, receiver = sizes[1:1 + 2 * twos:2], sizes[2:2 + 2 * twos:2]
    slack = jnp.minimum(source_of - 1, bound - receiver)
    moved = jax.random.randint(jax.random.fold_in(own_key, 1), (twos,), 0, 1 << 20) % (slack + 1)
    sizes = sizes.at[1:1 + 2 * twos:2].set(source_of - moved).at[2:2 + 2 * twos:2].set(receiver + moved)
    return sizes[jax.random.permutation(jax.random.fold_in(own_key, 2), number_of)]


def setup_inputs(seed: int = 0) -> dict:
    arg_keys = jax.random.split(jax.random.key(seed), 9)
    return {
        "teacher_states": draw_teacher_states(jax.random.fold_in(arg_keys[8], 71), 0),
        "student_states": draw_student_states(jax.random.fold_in(arg_keys[8], 71), 0),
        "teacher_gain": jnp.clip(1.0 + 0.15 * jax.random.normal(arg_keys[2], (DT,), jnp.float32), 0.25, 1.75),
        "student_gain": jnp.clip(1.0 + 0.15 * jax.random.normal(arg_keys[3], (DS,), jnp.float32), 0.25, 1.75),
        "mentor_output_weights": draw_mentor_output_weights(jax.random.fold_in(arg_keys[8], 71), 0),
        "student_heads": draw_student_heads(jax.random.fold_in(arg_keys[8], 71), 0),
        "segments": jax.vmap(lambda own: jnp.searchsorted(jnp.cumsum(ragged(own, DOCS, SEQUENCE_STEPS, 2 * ROW_DEV, 2)), jnp.arange(SEQUENCE_STEPS), side="right"))(jax.random.split(arg_keys[6], N_DP)).reshape((N_DP, SEQUENCE_STEPS)).astype(jnp.int32),
        "targets": place_ends(jax.random.randint(arg_keys[7], (N_DP, SEQUENCE_STEPS, QUANTIZER_TOTAL), 0, CODE_ALPHABET), jax.random.fold_in(arg_keys[7], 1), 0, CODE_ALPHABET - 1).astype(jnp.int32),
    }


epsilon = 1e-06
sharpness_divisor = 2.0
blend_ratio = 0.5

def normalize(states, gain):
    values = states.astype(jnp.float32)
    factor = lax.rsqrt(lax.optimization_barrier(jnp.mean(values * values, axis=-1, keepdims=True)) + epsilon)
    return (values * factor * gain.astype(jnp.float32)).astype(jnp.bfloat16)

def project_books(rows, heads):
    return jnp.stack([jnp.dot(rows, heads[book], preferred_element_type=jnp.float32) for book in range(QUANTIZER_TOTAL)], axis=1)

def reference(teacher_states, student_states, teacher_gain, student_gain, mentor_output_weights, student_heads, segments, targets):
    teacher_rows = []
    learner_sample_slab = []
    gradient = jnp.zeros((QUANTIZER_TOTAL, DS, CODE_ALPHABET), jnp.float32)
    for sequence in range(N_DP):
        picked_code_index = jax.nn.one_hot(targets[sequence], CODE_ALPHABET, dtype=jnp.float32)
        mentor_unit_scaled = normalize(teacher_states[sequence], teacher_gain)
        mentor_activations = project_books(mentor_unit_scaled, mentor_output_weights) / sharpness_divisor
        teacher_logp = mentor_activations - jax.nn.logsumexp(mentor_activations, axis=-1, keepdims=True)
        teacher_rows.append(-lax.optimization_barrier(jnp.sum(picked_code_index * teacher_logp, axis=-1)))
        teacher_sent = lax.optimization_barrier(teacher_logp.astype(jnp.bfloat16)).astype(jnp.float32)
        student_normed = normalize(student_states[sequence], student_gain)
        learner_activations = project_books(student_normed, student_heads)
        untempered_logdensity = learner_activations - jax.nn.logsumexp(learner_activations, axis=-1, keepdims=True)
        warmed_activations = learner_activations / sharpness_divisor
        warmed_logdensity = warmed_activations - jax.nn.logsumexp(warmed_activations, axis=-1, keepdims=True)
        mentor_distribution = jnp.exp(teacher_sent)
        kullback_gap = lax.optimization_barrier(jnp.sum(mentor_distribution * (teacher_sent - warmed_logdensity), axis=-1))
        mismatch_penalty = -lax.optimization_barrier(jnp.sum(picked_code_index * untempered_logdensity, axis=-1))
        learner_sample_slab.append(blend_ratio * sharpness_divisor * sharpness_divisor * kullback_gap + (1.0 - blend_ratio) * mismatch_penalty)
        members = (segments[sequence][None, :] == jnp.arange(DOCS, dtype=jnp.int32)[:, None]).astype(jnp.float32)
        counts = lax.optimization_barrier(jnp.sum(members, axis=1))
        row_sizes = jnp.dot(counts, members, precision=lax.Precision.HIGHEST)
        sample_importance = SEQUENCE_STEPS / (DOCS * row_sizes)
        gradient_scaling = sample_importance[:, None, None] * (blend_ratio * sharpness_divisor * (jnp.exp(warmed_logdensity) - mentor_distribution) + (1.0 - blend_ratio) * (jnp.exp(untempered_logdensity) - picked_code_index))
        gradient_scaling = gradient_scaling.astype(jnp.bfloat16)
        gradient = gradient + jnp.stack([lax.dot_general(student_normed, gradient_scaling[:, book], (((0,), (0,)), ((), ())), preferred_element_type=jnp.float32) for book in range(QUANTIZER_TOTAL)])
    frame_terms = jnp.stack([jnp.stack(teacher_rows), jnp.stack(learner_sample_slab)])
    return (gradient, frame_terms)
```

```python
import functools
import itertools

import jax
import jax.numpy as jnp
from jax import lax
from jax.experimental import pallas as pl
from jax.experimental.pallas import tpu as pltpu
from jax.sharding import PartitionSpec as P

epsilon = 1e-06
sharpness_divisor = 2.0
blend_ratio = 0.5
sub = 16
lanes = 128
pitch = 8

MESH = pl.DeviceIdType.MESH
f32 = jnp.float32
bf16 = jnp.bfloat16


def normalize_rows(source, gain, target, width):
    step = 512 if width % 512 == 0 else 128
    total = jnp.zeros((sub, step), f32)
    for start in range(0, width, step):
        x = source[:, start : start + step].astype(f32)
        total = total + x * x
    factor = lax.rsqrt(jnp.sum(total, axis=1, keepdims=True) / width + epsilon)
    for start in range(0, width, step):
        x = source[:, start : start + step].astype(f32)
        target[:, start : start + step] = (x * factor * gain[:, start : start + step]).astype(bf16)


def kernel(
    sizes,
    teacher_in,
    student_in,
    teacher_gain,
    student_gain,
    teacher_weights_in,
    student_weights_in,
    packed_in,
    out,
    terms_out,
    teacher_raw,
    student_raw,
    teacher_weights,
    student_weights,
    teacher_normed,
    student_normed,
    slabs,
    features_all,
    slopes_all,
    scaled,
    logits,
    packed,
    target_lanes,
    weight_lanes,
    stat_rows,
    stats,
    norm_rows,
    gaps,
    gaps_in,
    own_terms,
    swap,
    z_send,
    z_recv,
    z_local,
    weights_sem,
    packed_send,
    packed_recv,
    stats_send,
    stats_recv,
    feature_send,
    feature_recv,
    slope_send,
    slope_recv,
    gap_send,
    gap_recv,
    swap_sem,
):
    roles, dps, planes, inner, books, columns, share, half = sizes
    outer = dps // inner
    places = roles * dps
    rounds = half // sub
    group = planes * sub
    role = lax.axis_index("role")
    dp = lax.axis_index("dp")
    plane = lax.axis_index("ctx")
    ring, core = dp // inner, dp % inner
    me = role * dps + dp
    widths = (teacher_in.shape[1], student_in.shape[1])
    inputs = (teacher_in, student_in)
    raws = (teacher_raw, student_raw)
    middle = jnp.logical_and(plane > 0, plane < planes - 1)

    shifts = [s for s in itertools.product(range(roles), range(outer), range(inner))]

    def peer(shift, sign=1):
        dr, do, di = shift
        r = lax.rem(role + sign * dr + roles, roles)
        o = lax.rem(ring + sign * do + outer, outer)
        i = lax.rem(core + sign * di + inner, inner)
        return r, o * inner + i

    def place_of(where):
        return where[0] * dps + where[1]

    def rows(index, size):
        return pl.ds(pl.multiple_of(index * size, size), size)

    def remote(src, dst, send, recv, device):
        return pltpu.make_async_remote_copy(
            src_ref=src, dst_ref=dst, send_sem=send, recv_sem=recv, device_id=device, device_id_type=MESH
        )

    def z_copy(kind, s, b, up, own):
        src = inputs[kind].at[rows(role * rounds + s, sub)] if own else raws[kind].at[s, b]
        target = plane + 1 if up else plane - 1
        return remote(
            src, raws[kind].at[s, b], z_send.at[int(up), kind, s, b], z_recv.at[kind, s, b], (role, dp, target)
        )

    def send_own(kind, s):
        @pl.when(plane < planes - 1)
        def _():
            z_copy(kind, s, plane, True, True).start()

        @pl.when(plane > 0)
        def _():
            z_copy(kind, s, plane, False, True).start()

    def z_arrive(kind, s, b):
        z_copy(kind, s, b, True, False).wait_recv()

    def pass_on(kind, s, hop):
        @pl.when(jnp.logical_and(middle, plane - hop >= 0))
        def _():
            b = plane - hop
            z_arrive(kind, s, b)
            z_copy(kind, s, b, True, False).start()

        @pl.when(jnp.logical_and(middle, plane + hop <= planes - 1))
        def _():
            b = plane + hop
            z_arrive(kind, s, b)
            z_copy(kind, s, b, False, False).start()

    def forward(s):
        for kind in range(2):
            pass_on(kind, s, 1)

            @pl.when(s + 2 < rounds)
            def _():
                send_own(kind, s + 2)

            def hops(h, carry):
                pass_on(kind, s, h)
                return carry

            if planes > 2:
                lax.fori_loop(2, planes, hops, 0)

    def own_local(kind, s):
        return pltpu.make_async_copy(
            inputs[kind].at[rows(role * rounds + s, sub)], raws[kind].at[s, plane], z_local.at[kind, s]
        )

    def weight_copy(kind, q):
        src, dst = ((teacher_weights_in, teacher_weights), (student_weights_in, student_weights))[kind]
        return pltpu.make_async_copy(src.at[q], dst.at[q], weights_sem.at[kind, q])

    def packed_copy(step, arriving):
        other = lax.rem(plane + (planes - step if arriving else step), planes)
        slot = other if arriving else plane
        return remote(
            packed.at[slot] if arriving else packed_in,
            packed.at[slot],
            packed_send.at[step],
            packed_recv.at[slot],
            (role, dp, other),
        )

    def stats_copy(s, step, arriving):
        other = lax.rem(plane + (planes - step if arriving else step), planes)
        slot = other if arriving else plane
        return remote(
            stats.at[s, slot], stats.at[s, slot], stats_send.at[s, step], stats_recv.at[s, slot], (role, dp, other)
        )

    def gap_copy(step, arriving):
        other = lax.rem(plane + (planes - step if arriving else step), planes)
        slot = other if arriving else plane
        return remote(
            gaps.at[other], gaps_in.at[slot], gap_send.at[step], gap_recv.at[slot], (role, dp, other)
        )

    def feature_copy(s, n, arriving):
        where = peer(shifts[n], -1 if arriving else 1)
        there = place_of(where)
        slot = there if arriving else me
        return remote(
            slabs.at[s, there],
            features_all.at[s, rows(slot, group)],
            feature_send.at[s, n],
            feature_recv.at[s, slot],
            (where[0], where[1], plane),
        )

    def slope_copy(s, source, index, where):
        part = slopes_all.at[s, rows(source, group)]
        return remote(part, part, slope_send.at[s, index], slope_recv.at[s, source], (where[0], where[1], plane))

    faces = [(dr, do, 0) for dr, do in itertools.product(range(roles), range(outer)) if dr or do]
    cores = [(0, 0, di) for di in range(1, inner)]

    def over(count, body):
        def step(i, carry):
            body(i)
            return carry

        lax.fori_loop(0, count, step, 0)

    def project(kind, s, q):
        @pl.when(s == 0)
        def _():
            weight_copy(kind, q).wait()

        if kind == 0:
            scaled[q] = (
                jnp.dot(teacher_normed[...], teacher_weights[q], preferred_element_type=f32) / sharpness_divisor
            )
        else:
            logits[q] = jnp.dot(student_normed[...], student_weights[q], preferred_element_type=f32)

    def take(kind, s, b):
        @pl.when(b == plane)
        def _():
            own_local(kind, s).wait()

        @pl.when(jnp.logical_and(b != plane, jnp.logical_not(middle)))
        def _():
            z_arrive(kind, s, b)

        gain = (teacher_gain, student_gain)[kind]
        target = (teacher_normed, student_normed)[kind]
        normalize_rows(raws[kind].at[s, b], gain, target.at[rows(b, sub)], widths[kind])

    lane_of = lambda count: lax.broadcasted_iota(jnp.int32, (count, lanes), 1)

    def compute_logits(s):
        over(planes, lambda b: take(0, s, b))
        over(books, lambda q: project(0, s, q))
        over(planes, lambda b: take(1, s, b))

        def cut(b):
            for p in range(places):
                slabs[s, p, rows(b, sub), :] = student_normed[rows(b, sub), p * share : (p + 1) * share]

        over(planes, cut)
        features_all[s, rows(me, group), :] = slabs[s, me]
        over(books, lambda q: project(1, s, q))
        for n in range(1, places):
            feature_copy(s, n, False).start()

        positions = lax.broadcasted_iota(jnp.int32, (sub, columns), 1)
        lane = lane_of(sub)

        def totals(b):
            here = rows(b, sub)
            first = jnp.zeros((sub, lanes), f32)
            second = jnp.zeros((sub, lanes), f32)
            for q in range(books):
                hit = positions == target_lanes[s, here, q : q + 1]

                def put(array, kind, value):
                    return jnp.where(lane == kind * pitch + q, value, array)

                z = scaled[q, here, :]
                peak = jnp.max(z, axis=1, keepdims=True)
                first = put(first, 0, peak)
                first = put(first, 1, jnp.sum(jnp.exp(z - peak), axis=1, keepdims=True))
                first = put(first, 2, jnp.sum(jnp.where(hit, z, 0.0), axis=1, keepdims=True))
                u = logits[q, here, :]
                peak = jnp.max(u, axis=1, keepdims=True)
                centered = u - peak
                second = put(second, 0, peak)
                second = put(second, 1, jnp.sum(jnp.exp(centered), axis=1, keepdims=True))
                second = put(
                    second, 2, jnp.sum(jnp.exp(centered / sharpness_divisor), axis=1, keepdims=True)
                )
                second = put(second, 3, jnp.sum(jnp.where(hit, u, 0.0), axis=1, keepdims=True))
            stat_rows[here, :] = first
            stat_rows[rows(planes + b, sub), :] = second

        over(planes, totals)
        stats[s, plane] = jnp.transpose(stat_rows[...])[: 4 * pitch]

        def share_stats(step, carry):
            stats_copy(s, step, False).start()
            return carry

        lax.fori_loop(1, planes, share_stats, 0)

    def compute_slopes(s):
        def arrive(step, carry):
            stats_copy(s, step, True).wait_recv()
            return carry

        lax.fori_loop(1, planes, arrive, 0)

        def part(p, kind):
            return stats[s, p, kind * pitch : (kind + 1) * pitch, :]

        largest = lax.fori_loop(1, planes, lambda p, m: jnp.maximum(m, part(p, 0)), part(0, 0))

        def merge(p, carry):
            plain, warm, teacher_pick, student_pick = carry
            below = part(p, 0) - largest
            return (
                plain + part(p, 1) * jnp.exp(below),
                warm + part(p, 2) * jnp.exp(below / sharpness_divisor),
                teacher_pick + part(p, 2),
                student_pick + part(p, 3),
            )

        zero = jnp.zeros((pitch, 2 * group), f32)
        plain, warm, teacher_pick, student_pick = lax.fori_loop(0, planes, merge, (zero,) * 4)
        is_teacher = lax.broadcasted_iota(jnp.int32, (pitch, 2 * group), 1) < group
        plain_norm = largest + jnp.log(plain)
        warm_norm = largest / sharpness_divisor + jnp.log(jnp.where(is_teacher, 1.0, warm))
        term = plain_norm - jnp.where(is_teacher, teacher_pick, student_pick)
        merged = jnp.concatenate(
            [plain_norm, warm_norm, term, jnp.zeros((lanes - 3 * pitch, 2 * group), f32)], axis=0
        )
        norm_rows[...] = jnp.transpose(merged)
        own_terms[0, rows(s, sub), :] = norm_rows[rows(plane, sub), :]
        own_terms[1, rows(s, sub), :] = norm_rows[rows(planes + plane, sub), :]

        positions = lax.broadcasted_iota(jnp.int32, (sub, columns), 1)
        lane = lane_of(sub)

        def slope_rows(b):
            here = rows(b, sub)
            teacher_side = norm_rows[here, :]
            student_side = norm_rows[rows(planes + b, sub), :]
            weight = weight_lanes[s, here, :1]
            gap = jnp.zeros((sub, lanes), f32)
            for q in range(books):
                hit = positions == target_lanes[s, here, q : q + 1]
                teacher_logp = (scaled[q, here, :] - teacher_side[:, q : q + 1]).astype(bf16).astype(f32)
                mentor = jnp.exp(teacher_logp)
                u = logits[q, here, :]
                warmed = u / sharpness_divisor - student_side[:, pitch + q : pitch + q + 1]
                untempered = u - student_side[:, q : q + 1]
                value = jnp.sum(mentor * (teacher_logp - warmed), axis=1, keepdims=True)
                gap = jnp.where(lane == 2 * pitch + q, value, gap)
                slope = weight * (
                    blend_ratio * sharpness_divisor * (jnp.exp(warmed) - mentor)
                    + (1.0 - blend_ratio) * (jnp.exp(untempered) - jnp.where(hit, 1.0, 0.0))
                )
                slopes_all[
                    s, rows(me * planes + b, sub), q * columns : (q + 1) * columns
                ] = slope.astype(bf16)
            gaps[b, rows(s, sub), :] = gap

        over(planes, slope_rows)
        for index, shift in enumerate(faces + cores):
            slope_copy(s, me, index, peer(shift)).start()

    def relay_slopes(s):
        for n, shift in enumerate(faces):
            source = place_of(peer(shift, -1))
            slope_copy(s, source, 0, (role, dp)).wait_recv()
            for m, turn in enumerate(cores):
                index = len(faces) + len(cores) + n * len(cores) + m
                slope_copy(s, source, index, peer(turn)).start()

    def add_gradient(s):
        for n in range(1, places):
            feature_copy(s, n, True).wait_recv()
            if shifts[n][2]:
                slope_copy(s, place_of(peer(shifts[n], -1)), 0, (role, dp)).wait_recv()

        def book(q):
            out[q] = out[q] + lax.dot_general(
                features_all[s],
                slopes_all[s, :, rows(q, columns)],
                (((0,), (0,)), ((), ())),
                preferred_element_type=f32,
            )

        over(books, book)

    barrier = pltpu.get_barrier_semaphore()

    def greet(step, carry):
        other = lax.rem(plane + step, planes)
        pl.semaphore_signal(barrier, inc=1, device_id=(role, dp, other), device_id_type=MESH)
        return carry

    lax.fori_loop(1, planes, greet, 0)
    for shift in shifts[1:]:
        r, d = peer(shift)
        pl.semaphore_signal(barrier, inc=1, device_id=(r, d, plane), device_id_type=MESH)
    pl.semaphore_wait(barrier, planes - 1 + places - 1)

    def send_packed(step, carry):
        packed_copy(step, False).start()
        return carry

    lax.fori_loop(1, planes, send_packed, 0)
    for s in range(min(2, rounds)):
        for kind in range(2):
            send_own(kind, s)
    for kind in range(2):
        over(rounds, lambda s: own_local(kind, s).start())
    for kind in range(2):
        over(books, lambda q: weight_copy(kind, q).start())

    packed[plane] = packed_in[...]

    def clear(q):
        out[q] = jnp.zeros(out.shape[1:], f32)

    over(books, clear)

    def packed_arrive(step, carry):
        packed_copy(step, True).wait_recv()
        return carry

    lax.fori_loop(1, planes, packed_arrive, 0)
    length = packed.shape[2]
    picks = (
        lax.broadcasted_iota(jnp.int32, (half, length), 1)
        == lax.broadcasted_iota(jnp.int32, (half, length), 0) + role * half
    )

    def unpack(b):
        block = packed[b].astype(f32)

        def column(k):
            return jnp.sum(jnp.where(picks, block[k : k + 1, :], 0.0), axis=1, keepdims=True)

        lane = lane_of(half)
        ids = jnp.zeros((half, lanes), jnp.int32)
        for q in range(books):
            ids = jnp.where(lane == q, column(q).astype(jnp.int32) - plane * columns, ids)
        document = column(books)

        def count(p, total):
            same = document == packed[p].astype(f32)[books : books + 1, :]
            return total + jnp.sum(jnp.where(same, 1.0, 0.0), axis=1, keepdims=True)

        size = lax.fori_loop(0, planes, count, jnp.zeros((half, 1), f32))
        weight = jnp.broadcast_to((planes * length) / ((2 * planes) * size), (half, lanes))
        for s in range(rounds):
            target_lanes[s, rows(b, sub), :] = ids[s * sub : (s + 1) * sub]
            weight_lanes[s, rows(b, sub), :] = weight[s * sub : (s + 1) * sub]

    over(planes, unpack)

    forward(0)

    def iteration(s):
        @pl.when(s + 1 < rounds)
        def _():
            forward(s + 1)

        @pl.when(jnp.logical_and(s >= 1, s <= rounds))
        def _():
            compute_slopes(s - 1)

        @pl.when(s < rounds)
        def _():
            compute_logits(s)

        @pl.when(s >= 2)
        def _():
            add_gradient(s - 2)

        @pl.when(jnp.logical_and(s >= 1, s <= rounds))
        def _():
            relay_slopes(s - 1)

        @pl.when(s == rounds)
        def _():
            def send_gaps(step, carry):
                gap_copy(step, False).start()
                return carry

            lax.fori_loop(1, planes, send_gaps, 0)

    over(rounds + 2, iteration)

    def add_gap(step, total):
        gap_copy(step, True).wait_recv()
        return total + gaps_in[lax.rem(plane + planes - step, planes)]

    gap_total = lax.fori_loop(1, planes, add_gap, gaps[plane])
    student_terms = (
        blend_ratio * sharpness_divisor * sharpness_divisor * gap_total + (1.0 - blend_ratio) * own_terms[1]
    )
    teacher_terms = own_terms[0]
    mine = jnp.where(role == 0, teacher_terms, student_terms)
    swap[...] = jnp.where(role == 0, student_terms, teacher_terms)
    exchange = remote(swap, terms_out.at[role], swap_sem.at[0], swap_sem.at[1], (1 - role, dp, plane))
    exchange.start()
    terms_out[role] = mine
    exchange.wait_send()
    remote(swap, terms_out.at[1 - role], swap_sem.at[0], swap_sem.at[1], (1 - role, dp, plane)).wait_recv()

    def drain_line(step, carry):
        packed_copy(step, False).wait_send()
        gap_copy(step, False).wait_send()
        over(rounds, lambda s: stats_copy(s, step, False).wait_send())
        return carry

    lax.fori_loop(1, planes, drain_line, 0)

    def drain_round(s):
        for n in range(1, places):
            feature_copy(s, n, False).wait_send()
        for index in range(len(faces) + len(cores) + len(faces) * len(cores)):
            slope_copy(s, me, index, (role, dp)).wait_send()

        def drain_block(b):
            for kind in range(2):

                @pl.when(jnp.logical_and(b <= plane, plane < planes - 1))
                def _():
                    z_copy(kind, s, b, True, False).wait_send()

                @pl.when(jnp.logical_and(b >= plane, plane > 0))
                def _():
                    z_copy(kind, s, b, False, False).wait_send()

        over(planes, drain_block)

    over(rounds, drain_round)


def on_device(
    teacher_states,
    student_states,
    teacher_gain,
    student_gain,
    mentor_output_weights,
    student_heads,
    segments,
    targets,
):
    books, teacher_width, columns = mentor_output_weights.shape
    student_width = student_heads.shape[1]
    roles, dps, planes = (lax.axis_size(name) for name in ("role", "dp", "ctx"))
    inner = 2 if dps % 2 == 0 else 1
    places = roles * dps
    rows_here = teacher_states.shape[1]
    half = rows_here // roles
    rounds = half // sub
    group = planes * sub
    share = student_width // places
    sizes = (roles, dps, planes, inner, books, columns, share, half)

    packed = jnp.concatenate([targets[0].T, segments], axis=0)
    packed = jnp.pad(packed, ((0, pitch - books - 1), (0, 0)))

    vmem = pl.BlockSpec(memory_space=pltpu.VMEM)
    hbm = pl.BlockSpec(memory_space=pltpu.HBM)
    dma = pltpu.SemaphoreType.DMA
    shares, terms = pl.pallas_call(
        functools.partial(kernel, sizes),
        out_shape=(
            jax.ShapeDtypeStruct((books, share, columns), f32),
            jax.ShapeDtypeStruct((roles, half, lanes), f32),
        ),
        in_specs=[hbm, hbm, vmem, vmem, hbm, hbm, vmem],
        out_specs=(vmem, vmem),
        scratch_shapes=[
            pltpu.VMEM((rounds, planes, sub, teacher_width), bf16),
            pltpu.VMEM((rounds, planes, sub, student_width), bf16),
            pltpu.VMEM(mentor_output_weights.shape, bf16),
            pltpu.VMEM(student_heads.shape, bf16),
            pltpu.VMEM((group, teacher_width), bf16),
            pltpu.VMEM((group, student_width), bf16),
            pltpu.VMEM((rounds, places, group, share), bf16),
            pltpu.VMEM((rounds, places * group, share), bf16),
            pltpu.VMEM((rounds, places * group, books * columns), bf16),
            pltpu.VMEM((books, group, columns), f32),
            pltpu.VMEM((books, group, columns), f32),
            pltpu.VMEM((planes, pitch, rows_here), jnp.int32),
            pltpu.VMEM((rounds, group, lanes), jnp.int32),
            pltpu.VMEM((rounds, group, lanes), f32),
            pltpu.VMEM((2 * group, lanes), f32),
            pltpu.VMEM((rounds, planes, 4 * pitch, 2 * group), f32),
            pltpu.VMEM((2 * group, lanes), f32),
            pltpu.VMEM((planes, half, lanes), f32),
            pltpu.VMEM((planes, half, lanes), f32),
            pltpu.VMEM((2, half, lanes), f32),
            pltpu.VMEM((half, lanes), f32),
            dma((2, 2, rounds, planes)),
            dma((2, rounds, planes)),
            dma((2, rounds)),
            dma((2, books)),
            dma((planes,)),
            dma((planes,)),
            dma((rounds, planes)),
            dma((rounds, planes)),
            dma((rounds, places)),
            dma((rounds, places)),
            dma((rounds, places)),
            dma((rounds, places)),
            dma((planes,)),
            dma((planes,)),
            dma((2,)),
        ],
        compiler_params=pltpu.CompilerParams(
            collective_id=0, has_side_effects=True, vmem_limit_bytes=67_043_328
        ),
        name="distill",
    )(
        teacher_states[0],
        student_states[0],
        teacher_gain[None],
        student_gain[None],
        mentor_output_weights,
        student_heads,
        packed,
    )
    frame_terms = terms[:, :, 2 * pitch : 2 * pitch + books]
    return shares, frame_terms.reshape(1, 1, rows_here, books)


def solution(mesh):
    return jax.shard_map(
        on_device,
        mesh=mesh,
        in_specs=(
            P("dp", "ctx", None),
            P("dp", "ctx", None),
            P(),
            P(),
            P(None, None, "ctx"),
            P(None, None, "ctx"),
            P("dp", "ctx"),
            P("dp", "ctx", None),
        ),
        out_specs=(P(None, ("role", "dp"), "ctx"), P("role", "dp", "ctx", None)),
        check_vma=False,
    )
```

```python
import functools
import itertools

import jax
import jax.numpy as jnp
from jax import lax
from jax.experimental import pallas as pl
from jax.experimental.pallas import tpu as pltpu
from jax.sharding import PartitionSpec as P

epsilon = 1e-06
sharpness_divisor = 2.0
blend_ratio = 0.5
sub = 16
lanes = 128
pitch = 8

MESH = pl.DeviceIdType.MESH
f32 = jnp.float32
bf16 = jnp.bfloat16


def normalize_rows(source, gain, target, width):
    parts = [jnp.zeros((sub, lanes), f32) for _ in range(4)]
    for k in range(width // lanes):
        x = source[:, k * lanes : (k + 1) * lanes].astype(f32)
        parts[k % 4] = parts[k % 4] + x * x
    total = (parts[0] + parts[1]) + (parts[2] + parts[3])
    factor = lax.rsqrt(jnp.sum(total, axis=1, keepdims=True) / width + epsilon)
    for k in range(width // lanes):
        x = source[:, k * lanes : (k + 1) * lanes].astype(f32)
        target[:, k * lanes : (k + 1) * lanes] = (x * factor * gain[k : k + 1, :]).astype(bf16)


def kernel(
    sizes,
    teacher_in,
    student_in,
    teacher_gain,
    student_gain,
    teacher_weights_in,
    student_weights_in,
    targets_in,
    segments_in,
    out,
    terms_out,
    teacher_raw,
    student_raw,
    teacher_weights,
    student_weights,
    teacher_normed,
    student_normed,
    slabs,
    features_all,
    slopes_all,
    scaled,
    logits,
    targets_all,
    segments_all,
    target_lanes,
    weight_lanes,
    stat_rows,
    stats,
    norm_rows,
    gaps,
    gaps_in,
    own_terms,
    swap,
    both_terms,
    z_send,
    z_recv,
    z_local,
    weights_sem,
    packed_send,
    packed_recv,
    stats_send,
    stats_recv,
    feature_send,
    feature_recv,
    slope_send,
    slope_recv,
    gap_send,
    gap_recv,
    swap_sem,
):
    roles, dps, planes, inner, books, columns, share, half = sizes
    outer = dps // inner
    places = roles * dps
    rounds = half // sub
    group = planes * sub
    role = lax.axis_index("role")
    dp = lax.axis_index("dp")
    plane = lax.axis_index("ctx")
    ring, core = dp // inner, dp % inner
    me = role * dps + dp
    widths = (teacher_in.shape[1], student_in.shape[1])
    inputs = (teacher_in, student_in)
    raws = (teacher_raw, student_raw)
    middle = jnp.logical_and(plane > 0, plane < planes - 1)

    shifts = [s for s in itertools.product(range(roles), range(outer), range(inner))]

    def peer(shift, sign=1):
        dr, do, di = shift
        r = lax.rem(role + sign * dr + roles, roles)
        o = lax.rem(ring + sign * do + outer, outer)
        i = lax.rem(core + sign * di + inner, inner)
        return r, o * inner + i

    def place_of(where):
        return where[0] * dps + where[1]

    def rows(index, size):
        return pl.ds(pl.multiple_of(index * size, size), size)

    def remote(src, dst, send, recv, device):
        return pltpu.make_async_remote_copy(
            src_ref=src, dst_ref=dst, send_sem=send, recv_sem=recv, device_id=device, device_id_type=MESH
        )

    first, last = plane == 0, plane == planes - 1
    skips = planes > 2

    def z_copy(kind, s, b, up, own, distance=1):
        src = inputs[kind].at[rows(role * rounds + s, sub)] if own else raws[kind].at[s, b]
        target = plane + distance if up else plane - distance
        slot = int(up) if distance == 1 else 1 - int(up)
        return remote(
            src, raws[kind].at[s, b], z_send.at[slot, kind, s, b], z_recv.at[kind, s, b], (role, dp, target)
        )

    def passes(b, up):
        ahead = b < plane if up else b > plane
        inside = plane < planes - 1 if up else plane > 0
        edge = 0 if up else planes - 1
        direct = jnp.logical_and(b == edge, plane == (1 if up else planes - 2))
        relayed = jnp.logical_and(ahead, jnp.logical_not(direct)) if skips else ahead
        return jnp.logical_and(inside, relayed)

    def send_own(kind, s):
        @pl.when(jnp.logical_not(last))
        def _():
            z_copy(kind, s, plane, True, True).start()

        @pl.when(jnp.logical_not(first))
        def _():
            z_copy(kind, s, plane, False, True).start()

        if skips:

            @pl.when(first)
            def _():
                z_copy(kind, s, plane, True, True, 2).start()

            @pl.when(last)
            def _():
                z_copy(kind, s, plane, False, True, 2).start()

    def z_arrive(kind, s, b):
        z_copy(kind, s, b, True, False).wait_recv()

    def pass_on(kind, s, b, up):
        z_arrive(kind, s, b)

        @pl.when(passes(b, up))
        def _():
            z_copy(kind, s, b, up, False).start()

    def forward(s):
        for kind in range(2):

            def hops(h, carry):
                @pl.when(plane - h >= 0)
                def _():
                    pass_on(kind, s, plane - h, True)

                @pl.when(plane + h <= planes - 1)
                def _():
                    pass_on(kind, s, plane + h, False)

                return carry

            lax.fori_loop(1, planes, hops, 0)

    def own_local(kind, s):
        return pltpu.make_async_copy(
            inputs[kind].at[rows(role * rounds + s, sub)], raws[kind].at[s, plane], z_local.at[kind, s]
        )

    def weight_copy(kind, q):
        src, dst = ((teacher_weights_in, teacher_weights), (student_weights_in, student_weights))[kind]
        return pltpu.make_async_copy(src.at[q], dst.at[q], weights_sem.at[kind, q])

    labels = ((targets_in, targets_all), (segments_in, segments_all))

    def label_copy(n, step, arriving):
        other = lax.rem(plane + (planes - step if arriving else step), planes)
        slot = other if arriving else plane
        source, there = labels[n]
        return remote(source, there.at[slot], packed_send.at[n, step], packed_recv.at[n, slot], (role, dp, other))

    def stats_copy(s, step, arriving):
        other = lax.rem(plane + (planes - step if arriving else step), planes)
        slot = other if arriving else plane
        return remote(
            stats.at[s, slot], stats.at[s, slot], stats_send.at[s, step], stats_recv.at[s, slot], (role, dp, other)
        )

    def gap_copy(step, arriving):
        other = lax.rem(plane + (planes - step if arriving else step), planes)
        slot = other if arriving else plane
        return remote(
            gaps.at[other], gaps_in.at[slot], gap_send.at[step], gap_recv.at[slot], (role, dp, other)
        )

    def feature_copy(s, n, arriving):
        where = peer(shifts[n], -1 if arriving else 1)
        there = place_of(where)
        slot = there if arriving else me
        return remote(
            slabs.at[s, there],
            features_all.at[s, rows(slot, group)],
            feature_send.at[s, n],
            feature_recv.at[s, slot],
            (where[0], where[1], plane),
        )

    part_rows = group // 2

    def slope_copy(s, source, part, index, where):
        piece = slopes_all.at[s, rows(source * 2 + part, part_rows)]
        return remote(
            piece, piece, slope_send.at[s, index], slope_recv.at[s, source, part], (where[0], where[1], plane)
        )

    turns = [(0, 0, di) for di in range(1, inner)]
    across = [(dr, 0, 0) for dr in range(1, roles)]
    along = [(0, do, 0) for do in range(1, outer)]
    corners = [(dr, do, 0) for dr in range(1, roles) for do in range(1, outer)]
    own_sends = (
        [(t, 0) for t in across]
        + [(t, 1) for t in along]
        + [(t, 1) for t in across]
        + [(t, 0) for t in along]
        + [(t, h) for h in range(2) for t in turns]
    )
    slope_sends = (
        len(own_sends)
        + 2 * len(corners)
        + 2 * (len(across) + len(along) + len(corners)) * len(turns)
    )

    def over(count, body):
        def step(i, carry):
            body(i)
            return carry

        lax.fori_loop(0, count, step, 0)

    def project(kind, s, q):
        @pl.when(s == 0)
        def _():
            weight_copy(kind, q).wait()

        if kind == 0:
            scaled[q] = (
                jnp.dot(teacher_normed[...], teacher_weights[q], preferred_element_type=f32) / sharpness_divisor
            )
        else:
            logits[q] = jnp.dot(student_normed[...], student_weights[q], preferred_element_type=f32)

    def take(kind, s, b):
        @pl.when(b == plane)
        def _():
            own_local(kind, s).wait()

        @pl.when(jnp.logical_and(b != plane, jnp.logical_not(middle)))
        def _():
            z_arrive(kind, s, b)

        gain = (teacher_gain, student_gain)[kind]
        target = (teacher_normed, student_normed)[kind]
        normalize_rows(raws[kind].at[s, b], gain, target.at[rows(b, sub)], widths[kind])

    lane_of = lambda count: lax.broadcasted_iota(jnp.int32, (count, lanes), 1)

    def compute_logits(s):
        over(planes, lambda b: take(0, s, b))
        over(books, lambda q: project(0, s, q))
        over(planes, lambda b: take(1, s, b))

        def cut(b):
            for p in range(places):
                slabs[s, p, rows(b, sub), :] = student_normed[rows(b, sub), p * share : (p + 1) * share]

        over(planes, cut)
        features_all[s, rows(me, group), :] = slabs[s, me]
        over(books, lambda q: project(1, s, q))
        for n in range(1, places):
            feature_copy(s, n, False).start()

        positions = lax.broadcasted_iota(jnp.int32, (sub, columns), 1)
        lane = lane_of(sub)

        def totals(b):
            here = rows(b, sub)
            first = jnp.zeros((sub, lanes), f32)
            second = jnp.zeros((sub, lanes), f32)
            for q in range(books):
                hit = positions == target_lanes[s, here, q : q + 1]

                def put(array, kind, value):
                    return jnp.where(lane == kind * pitch + q, value, array)

                z = scaled[q, here, :]
                peak = jnp.max(z, axis=1, keepdims=True)
                first = put(first, 0, peak)
                first = put(first, 1, jnp.sum(jnp.exp(z - peak), axis=1, keepdims=True))
                first = put(first, 2, jnp.sum(jnp.where(hit, z, 0.0), axis=1, keepdims=True))
                u = logits[q, here, :]
                peak = jnp.max(u, axis=1, keepdims=True)
                centered = u - peak
                second = put(second, 0, peak)
                second = put(second, 1, jnp.sum(jnp.exp(centered), axis=1, keepdims=True))
                second = put(
                    second, 2, jnp.sum(jnp.exp(centered / sharpness_divisor), axis=1, keepdims=True)
                )
                second = put(second, 3, jnp.sum(jnp.where(hit, u, 0.0), axis=1, keepdims=True))
            stat_rows[here, :] = first
            stat_rows[rows(planes + b, sub), :] = second

        over(planes, totals)
        stats[s, plane] = jnp.transpose(stat_rows[...])[: 4 * pitch]

        def share_stats(step, carry):
            stats_copy(s, step, False).start()
            return carry

        lax.fori_loop(1, planes, share_stats, 0)

    def compute_slopes(s):
        def arrive(step, carry):
            stats_copy(s, step, True).wait_recv()
            return carry

        lax.fori_loop(1, planes, arrive, 0)

        def part(p, kind):
            return stats[s, p, kind * pitch : (kind + 1) * pitch, :]

        largest = lax.fori_loop(1, planes, lambda p, m: jnp.maximum(m, part(p, 0)), part(0, 0))

        def merge(p, carry):
            plain, warm, teacher_pick, student_pick = carry
            below = part(p, 0) - largest
            return (
                plain + part(p, 1) * jnp.exp(below),
                warm + part(p, 2) * jnp.exp(below / sharpness_divisor),
                teacher_pick + part(p, 2),
                student_pick + part(p, 3),
            )

        zero = jnp.zeros((pitch, 2 * group), f32)
        plain, warm, teacher_pick, student_pick = lax.fori_loop(0, planes, merge, (zero,) * 4)
        is_teacher = lax.broadcasted_iota(jnp.int32, (pitch, 2 * group), 1) < group
        plain_norm = largest + jnp.log(plain)
        warm_norm = largest / sharpness_divisor + jnp.log(jnp.where(is_teacher, 1.0, warm))
        term = plain_norm - jnp.where(is_teacher, teacher_pick, student_pick)
        merged = jnp.concatenate(
            [plain_norm, warm_norm, term, jnp.zeros((lanes - 3 * pitch, 2 * group), f32)], axis=0
        )
        norm_rows[...] = jnp.transpose(merged)
        own_terms[0, rows(s, sub), :] = norm_rows[rows(plane, sub), :]
        own_terms[1, rows(s, sub), :] = norm_rows[rows(planes + plane, sub), :]

        positions = lax.broadcasted_iota(jnp.int32, (sub, columns), 1)
        lane = lane_of(sub)

        def slope_rows(b):
            here = rows(b, sub)
            teacher_side = norm_rows[here, :]
            student_side = norm_rows[rows(planes + b, sub), :]
            weight = weight_lanes[s, here, :1]
            gap = jnp.zeros((sub, lanes), f32)
            for q in range(books):
                hit = positions == target_lanes[s, here, q : q + 1]
                teacher_logp = (scaled[q, here, :] - teacher_side[:, q : q + 1]).astype(bf16).astype(f32)
                mentor = jnp.exp(teacher_logp)
                u = logits[q, here, :]
                warmed = u / sharpness_divisor - student_side[:, pitch + q : pitch + q + 1]
                untempered = u - student_side[:, q : q + 1]
                value = jnp.sum(mentor * (teacher_logp - warmed), axis=1, keepdims=True)
                gap = jnp.where(lane == 2 * pitch + q, value, gap)
                slope = weight * (
                    blend_ratio * sharpness_divisor * (jnp.exp(warmed) - mentor)
                    + (1.0 - blend_ratio) * (jnp.exp(untempered) - jnp.where(hit, 1.0, 0.0))
                )
                slopes_all[
                    s, rows(me * planes + b, sub), q * columns : (q + 1) * columns
                ] = slope.astype(bf16)
            gaps[b, rows(s, sub), :] = gap

        over(planes, slope_rows)
        for index, (turn, part) in enumerate(own_sends):
            slope_copy(s, me, part, index, peer(turn)).start()

    def relay_slopes(s):
        index = len(own_sends)
        for lead in range(2):
            for turn in across + along:
                part = lead if turn in across else 1 - lead
                source = place_of(peer(turn, -1))
                slope_copy(s, source, part, 0, (role, dp)).wait_recv()
                if lead == 0:
                    for onward in along if turn in across else across:
                        slope_copy(s, source, part, index, peer(onward)).start()
                        index += 1
                for flip in turns:
                    slope_copy(s, source, part, index, peer(flip)).start()
                    index += 1

    def share_corners(s):
        index = slope_sends - 2 * len(corners) * len(turns)
        for turn in corners:
            source = place_of(peer(turn, -1))
            for part in range(2):
                slope_copy(s, source, part, 0, (role, dp)).wait_recv()
                for flip in turns:
                    slope_copy(s, source, part, index, peer(flip)).start()
                    index += 1

    def add_gradient(s):
        for n in range(1, places):
            feature_copy(s, n, True).wait_recv()
            if shifts[n][2]:
                for part in range(2):
                    slope_copy(s, place_of(peer(shifts[n], -1)), part, 0, (role, dp)).wait_recv()

        def book(q):
            out[q] = out[q] + lax.dot_general(
                features_all[s],
                slopes_all[s, :, rows(q, columns)],
                (((0,), (0,)), ((), ())),
                preferred_element_type=f32,
            )

        over(books, book)

    barrier = pltpu.get_barrier_semaphore()

    def greet(step, carry):
        other = lax.rem(plane + step, planes)
        pl.semaphore_signal(barrier, inc=1, device_id=(role, dp, other), device_id_type=MESH)
        return carry

    lax.fori_loop(1, planes, greet, 0)
    for shift in shifts[1:]:
        r, d = peer(shift)
        pl.semaphore_signal(barrier, inc=1, device_id=(r, d, plane), device_id_type=MESH)
    pl.semaphore_wait(barrier, planes - 1 + places - 1)

    def send_labels(step, carry):
        for n in range(2):
            label_copy(n, step, False).start()
        return carry

    lax.fori_loop(1, planes, send_labels, 0)
    for s in range(min(2, rounds)):
        for kind in range(2):
            send_own(kind, s)
    for kind in range(2):
        over(rounds, lambda s: own_local(kind, s).start())
    for kind in range(2):
        over(books, lambda q: weight_copy(kind, q).start())

    targets_all[plane] = targets_in[...]
    segments_all[plane] = segments_in[...]

    def clear(q):
        out[q] = jnp.zeros(out.shape[1:], f32)

    over(books, clear)

    def labels_arrive(step, carry):
        for n in range(2):
            label_copy(n, step, True).wait_recv()
        return carry

    lax.fori_loop(1, planes, labels_arrive, 0)
    length = segments_all.shape[2]
    picks = (
        lax.broadcasted_iota(jnp.int32, (half, length), 1)
        == lax.broadcasted_iota(jnp.int32, (half, length), 0) + role * half
    )

    def unpack(b):
        block = targets_all[b].astype(f32)

        def column(line):
            return jnp.sum(jnp.where(picks, line, 0.0), axis=1, keepdims=True)

        lane = lane_of(half)
        ids = jnp.zeros((half, lanes), jnp.int32)
        for q in range(books):
            ids = jnp.where(lane == q, column(block[q : q + 1, :]).astype(jnp.int32) - plane * columns, ids)
        document = column(segments_all[b].astype(f32))

        def count(p, total):
            same = document == segments_all[p].astype(f32)
            return total + jnp.sum(jnp.where(same, 1.0, 0.0), axis=1, keepdims=True)

        size = lax.fori_loop(0, planes, count, jnp.zeros((half, 1), f32))
        weight = jnp.broadcast_to((planes * length) / ((2 * planes) * size), (half, lanes))
        for s in range(rounds):
            target_lanes[s, rows(b, sub), :] = ids[s * sub : (s + 1) * sub]
            weight_lanes[s, rows(b, sub), :] = weight[s * sub : (s + 1) * sub]

    over(planes, unpack)

    def owns(s):
        for kind in range(2):
            send_own(kind, s)

    def between(low, s, high, also=True):
        return jnp.logical_and(jnp.logical_and(s >= low, s < high), also)

    def iteration(s):
        @pl.when(between(0, s, rounds, middle))
        def _():
            forward(s)

        @pl.when(between(1, s, rounds - 1, middle))
        def _():
            owns(s + 1)

        @pl.when(between(1, s, rounds + 1))
        def _():
            compute_slopes(s - 1)

        @pl.when(between(0, s, rounds))
        def _():
            compute_logits(s)

        @pl.when(between(0, s, rounds - 2, jnp.logical_not(middle)))
        def _():
            owns(s + 2)

        @pl.when(between(2, s, rounds + 2))
        def _():
            share_corners(s - 2)

        @pl.when(between(3, s, rounds + 3))
        def _():
            add_gradient(s - 3)

        @pl.when(s == rounds)
        def _():
            def send_gaps(step, carry):
                gap_copy(step, False).start()
                return carry

            lax.fori_loop(1, planes, send_gaps, 0)

        @pl.when(between(1, s, rounds + 1))
        def _():
            relay_slopes(s - 1)

    over(rounds + 3, iteration)

    def add_gap(step, total):
        gap_copy(step, True).wait_recv()
        return total + gaps_in[lax.rem(plane + planes - step, planes)]

    gap_total = lax.fori_loop(1, planes, add_gap, gaps[plane])
    student_terms = (
        blend_ratio * sharpness_divisor * sharpness_divisor * gap_total + (1.0 - blend_ratio) * own_terms[1]
    )
    teacher_terms = own_terms[0]
    mine = jnp.where(role == 0, teacher_terms, student_terms)
    swap[...] = jnp.where(role == 0, student_terms, teacher_terms)
    exchange = remote(swap, both_terms.at[rows(role, half)], swap_sem.at[0], swap_sem.at[1], (1 - role, dp, plane))
    exchange.start()
    both_terms[rows(role, half), :] = mine
    exchange.wait()
    terms_out[...] = jnp.transpose(both_terms[...])[2 * pitch : 2 * pitch + books]

    def drain_line(step, carry):
        for n in range(2):
            label_copy(n, step, False).wait_send()
        gap_copy(step, False).wait_send()
        over(rounds, lambda s: stats_copy(s, step, False).wait_send())
        return carry

    lax.fori_loop(1, planes, drain_line, 0)

    def drain_round(s):
        for n in range(1, places):
            feature_copy(s, n, False).wait_send()
        for index in range(slope_sends):
            slope_copy(s, me, 0, index, (role, dp)).wait_send()

        def drain_block(b):
            for kind in range(2):

                own = b == plane
                up = jnp.logical_or(passes(b, True), own if skips else jnp.logical_and(own, jnp.logical_not(last)))
                down = jnp.logical_or(passes(b, False), own if skips else jnp.logical_and(own, jnp.logical_not(first)))

                @pl.when(up)
                def _():
                    z_copy(kind, s, b, True, False).wait_send()

                @pl.when(down)
                def _():
                    z_copy(kind, s, b, False, False).wait_send()

        over(planes, drain_block)

    over(rounds, drain_round)


def on_device(
    teacher_states,
    student_states,
    teacher_gain,
    student_gain,
    mentor_output_weights,
    student_heads,
    segments,
    targets,
):
    books, teacher_width, columns = mentor_output_weights.shape
    student_width = student_heads.shape[1]
    roles, dps, planes = (lax.axis_size(name) for name in ("role", "dp", "ctx"))
    inner = 2 if dps % 2 == 0 else 1
    places = roles * dps
    rows_here = teacher_states.shape[1]
    half = rows_here // roles
    rounds = half // sub
    group = planes * sub
    share = student_width // places
    sizes = (roles, dps, planes, inner, books, columns, share, half)

    vmem = pl.BlockSpec(memory_space=pltpu.VMEM)
    hbm = pl.BlockSpec(memory_space=pltpu.HBM)
    dma = pltpu.SemaphoreType.DMA
    shares, terms = pl.pallas_call(
        functools.partial(kernel, sizes),
        out_shape=(
            jax.ShapeDtypeStruct((books, share, columns), f32),
            jax.ShapeDtypeStruct((books, rows_here), f32),
        ),
        in_specs=[hbm, hbm, vmem, vmem, hbm, hbm, vmem, vmem],
        out_specs=(vmem, vmem),
        scratch_shapes=[
            pltpu.VMEM((rounds, planes, sub, teacher_width), bf16),
            pltpu.VMEM((rounds, planes, sub, student_width), bf16),
            pltpu.VMEM(mentor_output_weights.shape, bf16),
            pltpu.VMEM(student_heads.shape, bf16),
            pltpu.VMEM((group, teacher_width), bf16),
            pltpu.VMEM((group, student_width), bf16),
            pltpu.VMEM((rounds, places, group, share), bf16),
            pltpu.VMEM((rounds, places * group, share), bf16),
            pltpu.VMEM((rounds, places * group, books * columns), bf16),
            pltpu.VMEM((books, group, columns), f32),
            pltpu.VMEM((books, group, columns), f32),
            pltpu.VMEM((planes, books, rows_here), jnp.int32),
            pltpu.VMEM((planes, 1, rows_here), jnp.int32),
            pltpu.VMEM((rounds, group, lanes), jnp.int32),
            pltpu.VMEM((rounds, group, lanes), f32),
            pltpu.VMEM((2 * group, lanes), f32),
            pltpu.VMEM((rounds, planes, 4 * pitch, 2 * group), f32),
            pltpu.VMEM((2 * group, lanes), f32),
            pltpu.VMEM((planes, half, lanes), f32),
            pltpu.VMEM((planes, half, lanes), f32),
            pltpu.VMEM((2, half, lanes), f32),
            pltpu.VMEM((half, lanes), f32),
            pltpu.VMEM((rows_here, lanes), f32),
            dma((2, 2, rounds, planes)),
            dma((2, rounds, planes)),
            dma((2, rounds)),
            dma((2, books)),
            dma((2, planes)),
            dma((2, planes)),
            dma((rounds, planes)),
            dma((rounds, planes)),
            dma((rounds, places)),
            dma((rounds, places)),
            dma((rounds, 4 * places)),
            dma((rounds, places, 2)),
            dma((planes,)),
            dma((planes,)),
            dma((2,)),
        ],
        compiler_params=pltpu.CompilerParams(
            collective_id=0, has_side_effects=True, vmem_limit_bytes=67_043_328
        ),
        name="distill",
    )(
        teacher_states[0],
        student_states[0],
        teacher_gain.reshape(-1, lanes),
        student_gain.reshape(-1, lanes),
        mentor_output_weights,
        student_heads,
        targets[0].T,
        segments,
    )
    return shares, terms.T.reshape(1, 1, rows_here, books)


def solution(mesh):
    return jax.shard_map(
        on_device,
        mesh=mesh,
        in_specs=(
            P("dp", "ctx", None),
            P("dp", "ctx", None),
            P(),
            P(),
            P(None, None, "ctx"),
            P(None, None, "ctx"),
            P("dp", "ctx"),
            P("dp", "ctx", None),
        ),
        out_specs=(P(None, ("role", "dp"), "ctx"), P("role", "dp", "ctx", None)),
        check_vma=False,
    )
```

```python
import functools
import itertools

import jax
import jax.numpy as jnp
from jax import lax
from jax.experimental import pallas as pl
from jax.experimental.pallas import tpu as pltpu
from jax.sharding import PartitionSpec as P

epsilon = 1e-06
sharpness_divisor = 2.0
blend_ratio = 0.5
sub = 16
lanes = 128
pitch = 8

MESH = pl.DeviceIdType.MESH
f32 = jnp.float32
bf16 = jnp.bfloat16


def normalize_rows(source, gain, target, width):
    parts = [jnp.zeros((sub, lanes), f32) for _ in range(4)]
    for k in range(width // lanes):
        x = source[:, k * lanes : (k + 1) * lanes].astype(f32)
        parts[k % 4] = parts[k % 4] + x * x
    total = (parts[0] + parts[1]) + (parts[2] + parts[3])
    factor = lax.rsqrt(jnp.sum(total, axis=1, keepdims=True) / width + epsilon)
    for k in range(width // lanes):
        x = source[:, k * lanes : (k + 1) * lanes].astype(f32)
        target[:, k * lanes : (k + 1) * lanes] = (x * factor * gain[k : k + 1, :]).astype(bf16)


def kernel(
    sizes,
    teacher_in,
    student_in,
    teacher_gain,
    student_gain,
    teacher_weights_in,
    student_weights_in,
    targets_in,
    segments_in,
    out,
    terms_out,
    teacher_raw,
    student_raw,
    teacher_weights,
    student_weights,
    teacher_normed,
    student_normed,
    slabs,
    features_all,
    slopes_all,
    scaled,
    logits,
    targets_all,
    segments_all,
    frame_lanes,
    stat_rows,
    stats,
    norm_rows,
    gaps,
    gaps_in,
    own_terms,
    swap,
    both_terms,
    features_turned,
    z_send,
    z_recv,
    z_local,
    weights_sem,
    packed_send,
    packed_recv,
    stats_send,
    stats_recv,
    feature_send,
    feature_recv,
    slope_send,
    slope_recv,
    gap_send,
    gap_recv,
    swap_sem,
):
    roles, dps, planes, inner, books, columns, share, half = sizes
    outer = dps // inner
    places = roles * dps
    rounds = half // sub
    group = planes * sub
    role = lax.axis_index("role")
    dp = lax.axis_index("dp")
    plane = lax.axis_index("ctx")
    ring, core = dp // inner, dp % inner
    me = role * dps + dp
    widths = (teacher_in.shape[1], student_in.shape[1])
    inputs = (teacher_in, student_in)
    raws = (teacher_raw, student_raw)
    middle = jnp.logical_and(plane > 0, plane < planes - 1)

    shifts = [s for s in itertools.product(range(roles), range(outer), range(inner))]

    def peer(shift, sign=1):
        dr, do, di = shift
        r = lax.rem(role + sign * dr + roles, roles)
        o = lax.rem(ring + sign * do + outer, outer)
        i = lax.rem(core + sign * di + inner, inner)
        return r, o * inner + i

    def place_of(where):
        return where[0] * dps + where[1]

    def rows(index, size):
        return pl.ds(pl.multiple_of(index * size, size), size)

    def remote(src, dst, send, recv, device):
        return pltpu.make_async_remote_copy(
            src_ref=src, dst_ref=dst, send_sem=send, recv_sem=recv, device_id=device, device_id_type=MESH
        )

    first, last = plane == 0, plane == planes - 1
    skips = planes > 2

    def z_copy(kind, s, b, up, own, distance=1):
        src = inputs[kind].at[rows(role * rounds + s, sub)] if own else raws[kind].at[s, b]
        target = plane + distance if up else plane - distance
        slot = int(up) if distance == 1 else 1 - int(up)
        return remote(
            src, raws[kind].at[s, b], z_send.at[slot, kind, s, b], z_recv.at[kind, s, b], (role, dp, target)
        )

    def passes(b, up):
        ahead = b < plane if up else b > plane
        inside = plane < planes - 1 if up else plane > 0
        edge = 0 if up else planes - 1
        direct = jnp.logical_and(b == edge, plane == (1 if up else planes - 2))
        relayed = jnp.logical_and(ahead, jnp.logical_not(direct)) if skips else ahead
        return jnp.logical_and(inside, relayed)

    def send_own(kind, s):
        @pl.when(jnp.logical_not(last))
        def _():
            z_copy(kind, s, plane, True, True).start()

        @pl.when(jnp.logical_not(first))
        def _():
            z_copy(kind, s, plane, False, True).start()

        if skips:

            @pl.when(first)
            def _():
                z_copy(kind, s, plane, True, True, 2).start()

            @pl.when(last)
            def _():
                z_copy(kind, s, plane, False, True, 2).start()

    def z_arrive(kind, s, b):
        z_copy(kind, s, b, True, False).wait_recv()

    def pass_on(kind, s, b, up):
        z_arrive(kind, s, b)

        @pl.when(passes(b, up))
        def _():
            z_copy(kind, s, b, up, False).start()

    def forward(kind, s):
        def hops(h, carry):
            @pl.when(plane - h >= 0)
            def _():
                pass_on(kind, s, plane - h, True)

            @pl.when(plane + h <= planes - 1)
            def _():
                pass_on(kind, s, plane + h, False)

            return carry

        lax.fori_loop(1, planes, hops, 0)

    def own_local(kind, s):
        return pltpu.make_async_copy(
            inputs[kind].at[rows(role * rounds + s, sub)], raws[kind].at[s, plane], z_local.at[kind, s]
        )

    def weight_copy(kind, q):
        src, dst = ((teacher_weights_in, teacher_weights), (student_weights_in, student_weights))[kind]
        return pltpu.make_async_copy(src.at[q], dst.at[q], weights_sem.at[kind, q])

    labels = ((targets_in, targets_all), (segments_in, segments_all))

    def label_copy(n, step, arriving):
        other = lax.rem(plane + (planes - step if arriving else step), planes)
        slot = other if arriving else plane
        source, there = labels[n]
        return remote(source, there.at[slot], packed_send.at[n, step], packed_recv.at[n, slot], (role, dp, other))

    def stats_copy(s, step, arriving):
        other = lax.rem(plane + (planes - step if arriving else step), planes)
        slot = other if arriving else plane
        return remote(
            stats.at[s, slot], stats.at[s, slot], stats_send.at[s, step], stats_recv.at[s, slot], (role, dp, other)
        )

    def gap_copy(step, arriving):
        other = lax.rem(plane + (planes - step if arriving else step), planes)
        slot = other if arriving else plane
        return remote(
            gaps.at[other], gaps_in.at[slot], gap_send.at[step], gap_recv.at[slot], (role, dp, other)
        )

    def feature_copy(s, n, arriving):
        where = peer(shifts[n], -1 if arriving else 1)
        there = place_of(where)
        slot = there if arriving else me
        return remote(
            slabs.at[s, there],
            features_all.at[s, rows(slot, group)],
            feature_send.at[s, n],
            feature_recv.at[s, slot],
            (where[0], where[1], plane),
        )

    part_rows = group // 2

    def slope_copy(s, source, part, index, where):
        piece = slopes_all.at[s, rows(source * 2 + part, part_rows)]
        return remote(
            piece, piece, slope_send.at[s, index], slope_recv.at[s, source, part], (where[0], where[1], plane)
        )

    turns = [(0, 0, di) for di in range(1, inner)]
    across = [(dr, 0, 0) for dr in range(1, roles)]
    along = [(0, do, 0) for do in range(1, outer)]
    corners = [(dr, do, 0) for dr in range(1, roles) for do in range(1, outer)]
    own_sends = (
        [(t, 0) for t in across]
        + [(t, 1) for t in along]
        + [(t, 1) for t in across]
        + [(t, 0) for t in along]
        + [(t, h) for h in range(2) for t in turns]
    )
    slope_sends = (
        len(own_sends)
        + 2 * len(corners)
        + 2 * (len(across) + len(along) + len(corners)) * len(turns)
    )

    def over(count, body):
        def step(i, carry):
            body(i)
            return carry

        lax.fori_loop(0, count, step, 0)

    def project(kind, s, q):
        @pl.when(s == 0)
        def _():
            weight_copy(kind, q).wait()

        if kind == 0:
            scaled[q] = (
                jnp.dot(teacher_normed[...], teacher_weights[q], preferred_element_type=f32) / sharpness_divisor
            )
        else:
            logits[q] = jnp.dot(student_normed[...], student_weights[q], preferred_element_type=f32)

    def take(kind, s, b):
        @pl.when(b == plane)
        def _():
            own_local(kind, s).wait()

        @pl.when(jnp.logical_and(b != plane, jnp.logical_not(middle)))
        def _():
            z_arrive(kind, s, b)

        gain = (teacher_gain, student_gain)[kind]
        target = (teacher_normed, student_normed)[kind]
        normalize_rows(raws[kind].at[s, b], gain, target.at[rows(b, sub)], widths[kind])

    lane_of = lambda count: lax.broadcasted_iota(jnp.int32, (count, lanes), 1)

    def teacher_logits(s):
        over(planes, lambda b: take(0, s, b))
        over(books, lambda q: project(0, s, q))

    def student_logits(s):
        over(planes, lambda b: take(1, s, b))

        def cut(b):
            for p in range(places):
                slabs[s, p, rows(b, sub), :] = student_normed[rows(b, sub), p * share : (p + 1) * share]

        over(planes, cut)
        for n in range(1, places):
            feature_copy(s, n, False).start()
        features_all[s, rows(me, group), :] = slabs[s, me]
        over(books, lambda q: project(1, s, q))

        positions = lax.broadcasted_iota(jnp.int32, (sub, columns), 1).astype(f32)
        lane = lane_of(sub)

        def totals(b):
            here = rows(b, sub)
            first = jnp.zeros((sub, lanes), f32)
            second = jnp.zeros((sub, lanes), f32)
            for q in range(books):
                hit = positions == frame_lanes[s, here, q : q + 1]

                def put(array, kind, value):
                    return jnp.where(lane == kind * pitch + q, value, array)

                z = scaled[q, here, :]
                peak = jnp.max(z, axis=1, keepdims=True)
                first = put(first, 0, peak)
                first = put(first, 1, jnp.sum(jnp.exp(z - peak), axis=1, keepdims=True))
                first = put(first, 2, jnp.sum(jnp.where(hit, z, 0.0), axis=1, keepdims=True))
                u = logits[q, here, :]
                peak = jnp.max(u, axis=1, keepdims=True)
                centered = u - peak
                second = put(second, 0, peak)
                second = put(second, 1, jnp.sum(jnp.exp(centered), axis=1, keepdims=True))
                second = put(
                    second, 2, jnp.sum(jnp.exp(centered / sharpness_divisor), axis=1, keepdims=True)
                )
                second = put(second, 3, jnp.sum(jnp.where(hit, u, 0.0), axis=1, keepdims=True))
            stat_rows[here, :] = first
            stat_rows[rows(planes + b, sub), :] = second

        over(planes, totals)
        stats[s, plane] = jnp.transpose(stat_rows[...])[: 4 * pitch]

        def share_stats(step, carry):
            stats_copy(s, step, False).start()
            return carry

        lax.fori_loop(1, planes, share_stats, 0)

    def compute_slopes(s):
        def arrive(step, carry):
            stats_copy(s, step, True).wait_recv()
            return carry

        lax.fori_loop(1, planes, arrive, 0)

        def part(p, kind):
            return stats[s, p, kind * pitch : (kind + 1) * pitch, :]

        largest = lax.fori_loop(1, planes, lambda p, m: jnp.maximum(m, part(p, 0)), part(0, 0))

        def merge(p, carry):
            plain, warm, teacher_pick, student_pick = carry
            below = part(p, 0) - largest
            return (
                plain + part(p, 1) * jnp.exp(below),
                warm + part(p, 2) * jnp.exp(below / sharpness_divisor),
                teacher_pick + part(p, 2),
                student_pick + part(p, 3),
            )

        zero = jnp.zeros((pitch, 2 * group), f32)
        plain, warm, teacher_pick, student_pick = lax.fori_loop(0, planes, merge, (zero,) * 4)
        is_teacher = lax.broadcasted_iota(jnp.int32, (pitch, 2 * group), 1) < group
        plain_norm = largest + jnp.log(plain)
        warm_norm = largest / sharpness_divisor + jnp.log(jnp.where(is_teacher, 1.0, warm))
        term = plain_norm - jnp.where(is_teacher, teacher_pick, student_pick)
        merged = jnp.concatenate(
            [plain_norm, warm_norm, term, jnp.zeros((lanes - 3 * pitch, 2 * group), f32)], axis=0
        )
        norm_rows[...] = jnp.transpose(merged)
        own_terms[0, rows(s, sub), :] = norm_rows[rows(plane, sub), :]
        own_terms[1, rows(s, sub), :] = norm_rows[rows(planes + plane, sub), :]

        positions = lax.broadcasted_iota(jnp.int32, (sub, columns), 1).astype(f32)
        lane = lane_of(sub)

        def slope_rows(b):
            here = rows(b, sub)
            teacher_side = norm_rows[here, :]
            student_side = norm_rows[rows(planes + b, sub), :]
            weight = frame_lanes[s, here, books : books + 1]
            gap = jnp.zeros((sub, lanes), f32)
            for q in range(books):
                hit = positions == frame_lanes[s, here, q : q + 1]
                teacher_logp = (scaled[q, here, :] - teacher_side[:, q : q + 1]).astype(bf16).astype(f32)
                mentor = jnp.exp(teacher_logp)
                u = logits[q, here, :]
                warmed = u / sharpness_divisor - student_side[:, pitch + q : pitch + q + 1]
                untempered = u - student_side[:, q : q + 1]
                value = jnp.sum(mentor * (teacher_logp - warmed), axis=1, keepdims=True)
                gap = jnp.where(lane == 2 * pitch + q, value, gap)
                slope = weight * (
                    blend_ratio * sharpness_divisor * (jnp.exp(warmed) - mentor)
                    + (1.0 - blend_ratio) * (jnp.exp(untempered) - jnp.where(hit, 1.0, 0.0))
                )
                slopes_all[
                    s, rows(me * planes + b, sub), q * columns : (q + 1) * columns
                ] = slope.astype(bf16)
            gaps[b, rows(s, sub), :] = gap

        over(planes, slope_rows)
        for index, (turn, part) in enumerate(own_sends):
            slope_copy(s, me, part, index, peer(turn)).start()

    def relay_slopes(s):
        index = len(own_sends)
        for lead in range(2):
            for turn in across + along:
                part = lead if turn in across else 1 - lead
                source = place_of(peer(turn, -1))
                slope_copy(s, source, part, 0, (role, dp)).wait_recv()
                if lead == 0:
                    for onward in along if turn in across else across:
                        slope_copy(s, source, part, index, peer(onward)).start()
                        index += 1
                for flip in turns:
                    slope_copy(s, source, part, index, peer(flip)).start()
                    index += 1

    def share_corners(s):
        index = slope_sends - 2 * len(corners) * len(turns)
        for turn in corners:
            source = place_of(peer(turn, -1))
            for part in range(2):
                slope_copy(s, source, part, 0, (role, dp)).wait_recv()
                for flip in turns:
                    slope_copy(s, source, part, index, peer(flip)).start()
                    index += 1

    def add_gradient(s):
        for n in range(1, places):
            feature_copy(s, n, True).wait_recv()
            if shifts[n][2]:
                for part in range(2):
                    slope_copy(s, place_of(peer(shifts[n], -1)), part, 0, (role, dp)).wait_recv()

        features_turned[...] = jnp.transpose(features_all[s])

        def book(q):
            out[q] = out[q] + jnp.dot(
                features_turned[...], slopes_all[s, :, rows(q, columns)], preferred_element_type=f32
            )

        over(books, book)

    barrier = pltpu.get_barrier_semaphore()

    def greet(step, carry):
        other = lax.rem(plane + step, planes)
        pl.semaphore_signal(barrier, inc=1, device_id=(role, dp, other), device_id_type=MESH)
        return carry

    lax.fori_loop(1, planes, greet, 0)
    for shift in shifts[1:]:
        r, d = peer(shift)
        pl.semaphore_signal(barrier, inc=1, device_id=(r, d, plane), device_id_type=MESH)
    pl.semaphore_wait(barrier, planes - 1 + places - 1)

    def send_labels(step, carry):
        for n in range(2):
            label_copy(n, step, False).start()
        return carry

    lax.fori_loop(1, planes, send_labels, 0)
    for s in range(min(2, rounds)):
        for kind in range(2):
            send_own(kind, s)
    for kind in range(2):
        over(rounds, lambda s: own_local(kind, s).start())
    for kind in range(2):
        over(books, lambda q: weight_copy(kind, q).start())

    targets_all[plane] = targets_in[...]
    segments_all[plane] = segments_in[...]

    def clear(q):
        out[q] = jnp.zeros(out.shape[1:], f32)

    over(books, clear)

    def labels_arrive(step, carry):
        for n in range(2):
            label_copy(n, step, True).wait_recv()
        return carry

    lax.fori_loop(1, planes, labels_arrive, 0)
    length = segments_all.shape[2]
    picks = (
        lax.broadcasted_iota(jnp.int32, (half, length), 1)
        == lax.broadcasted_iota(jnp.int32, (half, length), 0) + role * half
    )

    def unpack(b):
        block = targets_all[b].astype(f32)

        def column(line):
            return jnp.sum(jnp.where(picks, line, 0.0), axis=1, keepdims=True)

        lane = lane_of(half)
        facts = jnp.zeros((half, lanes), f32)
        first_column = (plane * columns).astype(f32)
        for q in range(books):
            facts = jnp.where(lane == q, column(block[q : q + 1, :]) - first_column, facts)
        document = column(segments_all[b].astype(f32))

        def count(p, total):
            same = document == segments_all[p].astype(f32)
            return total + jnp.sum(jnp.where(same, 1.0, 0.0), axis=1, keepdims=True)

        size = lax.fori_loop(0, planes, count, jnp.zeros((half, 1), f32))
        weight = (planes * length) / ((2 * planes) * size)
        facts = jnp.where(lane == books, weight, facts)
        for s in range(rounds):
            frame_lanes[s, rows(b, sub), :] = facts[s * sub : (s + 1) * sub]

    over(planes, unpack)

    def owns(s):
        for kind in range(2):
            send_own(kind, s)

    def between(low, s, high, also=True):
        return jnp.logical_and(jnp.logical_and(s >= low, s < high), also)

    @pl.when(middle)
    def _():
        for kind in range(2):
            forward(kind, 0)

    def iteration(s):
        @pl.when(between(1, s, rounds + 1))
        def _():
            compute_slopes(s - 1)

        @pl.when(between(0, s, rounds))
        def _():
            teacher_logits(s)

        @pl.when(between(0, s, rounds - 1, middle))
        def _():
            forward(0, s + 1)

        @pl.when(between(0, s, rounds))
        def _():
            student_logits(s)

        @pl.when(between(0, s, rounds - 1, middle))
        def _():
            forward(1, s + 1)

        @pl.when(between(0, s, rounds - 2))
        def _():
            owns(s + 2)

        @pl.when(s == rounds)
        def _():
            def send_gaps(step, carry):
                gap_copy(step, False).start()
                return carry

            lax.fori_loop(1, planes, send_gaps, 0)

        @pl.when(between(3, s, rounds + 3))
        def _():
            add_gradient(s - 3)

        @pl.when(between(2, s, rounds + 2))
        def _():
            share_corners(s - 2)

        @pl.when(between(1, s, rounds + 1))
        def _():
            relay_slopes(s - 1)

    over(rounds + 3, iteration)

    def add_gap(step, total):
        gap_copy(step, True).wait_recv()
        return total + gaps_in[lax.rem(plane + planes - step, planes)]

    gap_total = lax.fori_loop(1, planes, add_gap, gaps[plane])
    student_terms = (
        blend_ratio * sharpness_divisor * sharpness_divisor * gap_total + (1.0 - blend_ratio) * own_terms[1]
    )
    teacher_terms = own_terms[0]
    mine = jnp.where(role == 0, teacher_terms, student_terms)
    swap[...] = jnp.where(role == 0, student_terms, teacher_terms)
    exchange = remote(swap, both_terms.at[rows(role, half)], swap_sem.at[0], swap_sem.at[1], (1 - role, dp, plane))
    exchange.start()
    both_terms[rows(role, half), :] = mine
    exchange.wait()
    terms_out[...] = jnp.transpose(both_terms[...])[2 * pitch : 2 * pitch + books]

    def drain_line(step, carry):
        for n in range(2):
            label_copy(n, step, False).wait_send()
        gap_copy(step, False).wait_send()
        over(rounds, lambda s: stats_copy(s, step, False).wait_send())
        return carry

    lax.fori_loop(1, planes, drain_line, 0)

    def drain_round(s):
        for n in range(1, places):
            feature_copy(s, n, False).wait_send()
        for index in range(slope_sends):
            slope_copy(s, me, 0, index, (role, dp)).wait_send()

        def drain_block(b):
            for kind in range(2):

                own = b == plane
                up = jnp.logical_or(passes(b, True), own if skips else jnp.logical_and(own, jnp.logical_not(last)))
                down = jnp.logical_or(passes(b, False), own if skips else jnp.logical_and(own, jnp.logical_not(first)))

                @pl.when(up)
                def _():
                    z_copy(kind, s, b, True, False).wait_send()

                @pl.when(down)
                def _():
                    z_copy(kind, s, b, False, False).wait_send()

        over(planes, drain_block)

    over(rounds, drain_round)


def on_device(
    teacher_states,
    student_states,
    teacher_gain,
    student_gain,
    mentor_output_weights,
    student_heads,
    segments,
    targets,
):
    books, teacher_width, columns = mentor_output_weights.shape
    student_width = student_heads.shape[1]
    roles, dps, planes = (lax.axis_size(name) for name in ("role", "dp", "ctx"))
    inner = 2 if dps % 2 == 0 else 1
    places = roles * dps
    rows_here = teacher_states.shape[1]
    half = rows_here // roles
    rounds = half // sub
    group = planes * sub
    share = student_width // places
    sizes = (roles, dps, planes, inner, books, columns, share, half)

    vmem = pl.BlockSpec(memory_space=pltpu.VMEM)
    hbm = pl.BlockSpec(memory_space=pltpu.HBM)
    dma = pltpu.SemaphoreType.DMA
    shares, terms = pl.pallas_call(
        functools.partial(kernel, sizes),
        out_shape=(
            pltpu.VMEM((books, share, columns), f32),
            jax.ShapeDtypeStruct((books, rows_here), f32),
        ),
        in_specs=[hbm, hbm, vmem, vmem, hbm, hbm, vmem, vmem],
        out_specs=(vmem, vmem),
        scratch_shapes=[
            pltpu.VMEM((rounds, planes, sub, teacher_width), bf16),
            pltpu.VMEM((rounds, planes, sub, student_width), bf16),
            pltpu.VMEM(mentor_output_weights.shape, bf16),
            pltpu.VMEM(student_heads.shape, bf16),
            pltpu.VMEM((group, teacher_width), bf16),
            pltpu.VMEM((group, student_width), bf16),
            pltpu.VMEM((rounds, places, group, share), bf16),
            pltpu.VMEM((rounds, places * group, share), bf16),
            pltpu.VMEM((rounds, places * group, books * columns), bf16),
            pltpu.VMEM((books, group, columns), f32),
            pltpu.VMEM((books, group, columns), f32),
            pltpu.VMEM((planes, books, rows_here), jnp.int32),
            pltpu.VMEM((planes, 1, rows_here), jnp.int32),
            pltpu.VMEM((rounds, group, lanes), f32),
            pltpu.VMEM((2 * group, lanes), f32),
            pltpu.VMEM((rounds, planes, 4 * pitch, 2 * group), f32),
            pltpu.VMEM((2 * group, lanes), f32),
            pltpu.VMEM((planes, half, lanes), f32),
            pltpu.VMEM((planes, half, lanes), f32),
            pltpu.VMEM((2, half, lanes), f32),
            pltpu.VMEM((half, lanes), f32),
            pltpu.VMEM((rows_here, lanes), f32),
            pltpu.VMEM((share, places * group), bf16),
            dma((2, 2, rounds, planes)),
            dma((2, rounds, planes)),
            dma((2, rounds)),
            dma((2, books)),
            dma((2, planes)),
            dma((2, planes)),
            dma((rounds, planes)),
            dma((rounds, planes)),
            dma((rounds, places)),
            dma((rounds, places)),
            dma((rounds, 4 * places)),
            dma((rounds, places, 2)),
            dma((planes,)),
            dma((planes,)),
            dma((2,)),
        ],
        compiler_params=pltpu.CompilerParams(
            collective_id=0, has_side_effects=True, vmem_limit_bytes=67_043_328 - 4 * books * share * columns - (1 << 17)
        ),
        name="distill",
    )(
        teacher_states[0],
        student_states[0],
        teacher_gain.reshape(-1, lanes),
        student_gain.reshape(-1, lanes),
        mentor_output_weights,
        student_heads,
        targets[0].T,
        segments,
    )
    return shares, terms.T.reshape(1, 1, rows_here, books)


def solution(mesh):
    return jax.shard_map(
        on_device,
        mesh=mesh,
        in_specs=(
            P("dp", "ctx", None),
            P("dp", "ctx", None),
            P(),
            P(),
            P(None, None, "ctx"),
            P(None, None, "ctx"),
            P("dp", "ctx"),
            P("dp", "ctx", None),
        ),
        out_specs=(P(None, ("role", "dp"), "ctx"), P("role", "dp", "ctx", None)),
        check_vma=False,
    )
```

```python
import functools
import itertools

import jax
import jax.numpy as jnp
from jax import lax
from jax.experimental import pallas as pl
from jax.experimental.pallas import tpu as pltpu
from jax.sharding import PartitionSpec as P

epsilon = 1e-06
sharpness_divisor = 2.0
blend_ratio = 0.5
sub = 16
lanes = 128
pitch = 8

MESH = pl.DeviceIdType.MESH
f32 = jnp.float32
bf16 = jnp.bfloat16


def normalize_rows(source, gain, target, width):
    parts = [jnp.zeros((sub, lanes), f32) for _ in range(4)]
    for k in range(width // lanes):
        x = source[:, k * lanes : (k + 1) * lanes].astype(f32)
        parts[k % 4] = parts[k % 4] + x * x
    total = (parts[0] + parts[1]) + (parts[2] + parts[3])
    factor = lax.rsqrt(jnp.sum(total, axis=1, keepdims=True) / width + epsilon)
    for k in range(width // lanes):
        x = source[:, k * lanes : (k + 1) * lanes].astype(f32)
        target[:, k * lanes : (k + 1) * lanes] = (x * factor * gain[k : k + 1, :]).astype(bf16)


def kernel(
    sizes,
    teacher_in,
    student_in,
    teacher_gain,
    student_gain,
    teacher_weights_in,
    student_weights_in,
    targets_in,
    segments_in,
    out,
    terms_out,
    teacher_raw,
    student_raw,
    teacher_weights,
    student_weights,
    teacher_normed,
    student_normed,
    slabs,
    features_all,
    slopes_all,
    scaled,
    logits,
    targets_all,
    segments_all,
    target_lanes,
    weight_lanes,
    stat_rows,
    stats,
    norm_rows,
    gaps,
    gaps_in,
    own_terms,
    swap,
    both_terms,
    z_send,
    z_recv,
    z_local,
    weights_sem,
    packed_send,
    packed_recv,
    stats_send,
    stats_recv,
    feature_send,
    feature_recv,
    slope_send,
    slope_recv,
    gap_send,
    gap_recv,
    swap_sem,
):
    roles, dps, planes, inner, books, columns, share, half = sizes
    outer = dps // inner
    places = roles * dps
    rounds = half // sub
    group = planes * sub
    role = lax.axis_index("role")
    dp = lax.axis_index("dp")
    plane = lax.axis_index("ctx")
    ring, core = dp // inner, dp % inner
    me = role * dps + dp
    widths = (teacher_in.shape[1], student_in.shape[1])
    inputs = (teacher_in, student_in)
    raws = (teacher_raw, student_raw)
    middle = jnp.logical_and(plane > 0, plane < planes - 1)

    shifts = [s for s in itertools.product(range(roles), range(outer), range(inner))]

    def peer(shift, sign=1):
        dr, do, di = shift
        r = lax.rem(role + sign * dr + roles, roles)
        o = lax.rem(ring + sign * do + outer, outer)
        i = lax.rem(core + sign * di + inner, inner)
        return r, o * inner + i

    def place_of(where):
        return where[0] * dps + where[1]

    def rows(index, size):
        return pl.ds(pl.multiple_of(index * size, size), size)

    def remote(src, dst, send, recv, device):
        return pltpu.make_async_remote_copy(
            src_ref=src, dst_ref=dst, send_sem=send, recv_sem=recv, device_id=device, device_id_type=MESH
        )

    first, last = plane == 0, plane == planes - 1
    skips = planes > 2

    def z_copy(kind, s, b, up, own, distance=1):
        src = inputs[kind].at[rows(role * rounds + s, sub)] if own else raws[kind].at[s, b]
        target = plane + distance if up else plane - distance
        slot = int(up) if distance == 1 else 1 - int(up)
        return remote(
            src, raws[kind].at[s, b], z_send.at[slot, kind, s, b], z_recv.at[kind, s, b], (role, dp, target)
        )

    def passes(b, up):
        ahead = b < plane if up else b > plane
        inside = plane < planes - 1 if up else plane > 0
        edge = 0 if up else planes - 1
        direct = jnp.logical_and(b == edge, plane == (1 if up else planes - 2))
        relayed = jnp.logical_and(ahead, jnp.logical_not(direct)) if skips else ahead
        return jnp.logical_and(inside, relayed)

    def send_own(kind, s):
        @pl.when(jnp.logical_not(last))
        def _():
            z_copy(kind, s, plane, True, True).start()

        @pl.when(jnp.logical_not(first))
        def _():
            z_copy(kind, s, plane, False, True).start()

        if skips:

            @pl.when(first)
            def _():
                z_copy(kind, s, plane, True, True, 2).start()

            @pl.when(last)
            def _():
                z_copy(kind, s, plane, False, True, 2).start()

    def z_arrive(kind, s, b):
        z_copy(kind, s, b, True, False).wait_recv()

    def pass_on(kind, s, b, up):
        z_arrive(kind, s, b)

        @pl.when(passes(b, up))
        def _():
            z_copy(kind, s, b, up, False).start()

    def forward(kind, s):
        def hops(h, carry):
            @pl.when(plane - h >= 0)
            def _():
                pass_on(kind, s, plane - h, True)

            @pl.when(plane + h <= planes - 1)
            def _():
                pass_on(kind, s, plane + h, False)

            return carry

        lax.fori_loop(1, planes, hops, 0)

    def own_local(kind, s):
        return pltpu.make_async_copy(
            inputs[kind].at[rows(role * rounds + s, sub)], raws[kind].at[s, plane], z_local.at[kind, s]
        )

    def weight_copy(kind, q):
        src, dst = ((teacher_weights_in, teacher_weights), (student_weights_in, student_weights))[kind]
        return pltpu.make_async_copy(src.at[q], dst.at[q], weights_sem.at[kind, q])

    labels = ((targets_in, targets_all), (segments_in, segments_all))

    def label_copy(n, step, arriving):
        other = lax.rem(plane + (planes - step if arriving else step), planes)
        slot = other if arriving else plane
        source, there = labels[n]
        return remote(source, there.at[slot], packed_send.at[n, step], packed_recv.at[n, slot], (role, dp, other))

    def stats_copy(s, step, arriving):
        other = lax.rem(plane + (planes - step if arriving else step), planes)
        slot = other if arriving else plane
        return remote(
            stats.at[s, slot], stats.at[s, slot], stats_send.at[s, step], stats_recv.at[s, slot], (role, dp, other)
        )

    def gap_copy(step, arriving):
        other = lax.rem(plane + (planes - step if arriving else step), planes)
        slot = other if arriving else plane
        return remote(
            gaps.at[other], gaps_in.at[slot], gap_send.at[step], gap_recv.at[slot], (role, dp, other)
        )

    def feature_copy(s, n, arriving):
        where = peer(shifts[n], -1 if arriving else 1)
        there = place_of(where)
        slot = there if arriving else me
        return remote(
            slabs.at[s, there],
            features_all.at[s, rows(slot, group)],
            feature_send.at[s, n],
            feature_recv.at[s, slot],
            (where[0], where[1], plane),
        )

    part_rows = group // 2

    def slope_copy(s, source, part, index, where):
        piece = slopes_all.at[s, rows(source * 2 + part, part_rows)]
        return remote(
            piece, piece, slope_send.at[s, index], slope_recv.at[s, source, part], (where[0], where[1], plane)
        )

    turns = [(0, 0, di) for di in range(1, inner)]
    across = [(dr, 0, 0) for dr in range(1, roles)]
    along = [(0, do, 0) for do in range(1, outer)]
    corners = [(dr, do, 0) for dr in range(1, roles) for do in range(1, outer)]
    own_sends = (
        [(t, 0) for t in across]
        + [(t, 1) for t in along]
        + [(t, 1) for t in across]
        + [(t, 0) for t in along]
        + [(t, h) for h in range(2) for t in turns]
    )
    slope_sends = (
        len(own_sends)
        + 2 * len(corners)
        + 2 * (len(across) + len(along) + len(corners)) * len(turns)
    )

    def over(count, body):
        def step(i, carry):
            body(i)
            return carry

        lax.fori_loop(0, count, step, 0)

    def project(kind, s, q):
        @pl.when(s == 0)
        def _():
            weight_copy(kind, q).wait()

        if kind == 0:
            scaled[q] = (
                jnp.dot(teacher_normed[...], teacher_weights[q], preferred_element_type=f32) / sharpness_divisor
            )
        else:
            logits[q] = jnp.dot(student_normed[...], student_weights[q], preferred_element_type=f32)

    def take(kind, s, b):
        @pl.when(b == plane)
        def _():
            own_local(kind, s).wait()

        @pl.when(jnp.logical_and(b != plane, jnp.logical_not(middle)))
        def _():
            z_arrive(kind, s, b)

        gain = (teacher_gain, student_gain)[kind]
        target = (teacher_normed, student_normed)[kind]
        normalize_rows(raws[kind].at[s, b], gain, target.at[rows(b, sub)], widths[kind])

    lane_of = lambda count: lax.broadcasted_iota(jnp.int32, (count, lanes), 1)

    def teacher_logits(s):
        over(planes, lambda b: take(0, s, b))
        over(books, lambda q: project(0, s, q))

    def student_logits(s):
        over(planes, lambda b: take(1, s, b))

        def cut(b):
            for p in range(places):
                slabs[s, p, rows(b, sub), :] = student_normed[rows(b, sub), p * share : (p + 1) * share]

        over(planes, cut)
        for n in range(1, places):
            feature_copy(s, n, False).start()
        features_all[s, rows(me, group), :] = slabs[s, me]
        over(books, lambda q: project(1, s, q))

        positions = lax.broadcasted_iota(jnp.int32, (sub, columns), 1)
        lane = lane_of(sub)

        def totals(b):
            here = rows(b, sub)
            first = jnp.zeros((sub, lanes), f32)
            second = jnp.zeros((sub, lanes), f32)
            for q in range(books):
                hit = positions == target_lanes[s, here, q : q + 1]

                def put(array, kind, value):
                    return jnp.where(lane == kind * pitch + q, value, array)

                z = scaled[q, here, :]
                peak = jnp.max(z, axis=1, keepdims=True)
                first = put(first, 0, peak)
                first = put(first, 1, jnp.sum(jnp.exp(z - peak), axis=1, keepdims=True))
                first = put(first, 2, jnp.sum(jnp.where(hit, z, 0.0), axis=1, keepdims=True))
                u = logits[q, here, :]
                peak = jnp.max(u, axis=1, keepdims=True)
                centered = u - peak
                second = put(second, 0, peak)
                second = put(second, 1, jnp.sum(jnp.exp(centered), axis=1, keepdims=True))
                second = put(
                    second, 2, jnp.sum(jnp.exp(centered / sharpness_divisor), axis=1, keepdims=True)
                )
                second = put(second, 3, jnp.sum(jnp.where(hit, u, 0.0), axis=1, keepdims=True))
            stat_rows[here, :] = first
            stat_rows[rows(planes + b, sub), :] = second

        over(planes, totals)
        stats[s, plane] = jnp.transpose(stat_rows[...])[: 4 * pitch]

        def share_stats(step, carry):
            stats_copy(s, step, False).start()
            return carry

        lax.fori_loop(1, planes, share_stats, 0)

    def compute_slopes(s):
        def arrive(step, carry):
            stats_copy(s, step, True).wait_recv()
            return carry

        lax.fori_loop(1, planes, arrive, 0)

        def part(p, kind):
            return stats[s, p, kind * pitch : (kind + 1) * pitch, :]

        largest = lax.fori_loop(1, planes, lambda p, m: jnp.maximum(m, part(p, 0)), part(0, 0))

        def merge(p, carry):
            plain, warm, teacher_pick, student_pick = carry
            below = part(p, 0) - largest
            return (
                plain + part(p, 1) * jnp.exp(below),
                warm + part(p, 2) * jnp.exp(below / sharpness_divisor),
                teacher_pick + part(p, 2),
                student_pick + part(p, 3),
            )

        zero = jnp.zeros((pitch, 2 * group), f32)
        plain, warm, teacher_pick, student_pick = lax.fori_loop(0, planes, merge, (zero,) * 4)
        is_teacher = lax.broadcasted_iota(jnp.int32, (pitch, 2 * group), 1) < group
        plain_norm = largest + jnp.log(plain)
        warm_norm = largest / sharpness_divisor + jnp.log(jnp.where(is_teacher, 1.0, warm))
        term = plain_norm - jnp.where(is_teacher, teacher_pick, student_pick)
        merged = jnp.concatenate(
            [plain_norm, warm_norm, term, jnp.zeros((lanes - 3 * pitch, 2 * group), f32)], axis=0
        )
        norm_rows[...] = jnp.transpose(merged)
        own_terms[0, rows(s, sub), :] = norm_rows[rows(plane, sub), :]
        own_terms[1, rows(s, sub), :] = norm_rows[rows(planes + plane, sub), :]

        positions = lax.broadcasted_iota(jnp.int32, (sub, columns), 1)
        lane = lane_of(sub)

        def slope_rows(b):
            here = rows(b, sub)
            teacher_side = norm_rows[here, :]
            student_side = norm_rows[rows(planes + b, sub), :]
            weight = weight_lanes[s, here, :1]
            gap = jnp.zeros((sub, lanes), f32)
            for q in range(books):
                hit = positions == target_lanes[s, here, q : q + 1]
                teacher_logp = (scaled[q, here, :] - teacher_side[:, q : q + 1]).astype(bf16).astype(f32)
                mentor = jnp.exp(teacher_logp)
                u = logits[q, here, :]
                warmed = u / sharpness_divisor - student_side[:, pitch + q : pitch + q + 1]
                untempered = u - student_side[:, q : q + 1]
                value = jnp.sum(mentor * (teacher_logp - warmed), axis=1, keepdims=True)
                gap = jnp.where(lane == 2 * pitch + q, value, gap)
                slope = weight * (
                    blend_ratio * sharpness_divisor * (jnp.exp(warmed) - mentor)
                    + (1.0 - blend_ratio) * (jnp.exp(untempered) - jnp.where(hit, 1.0, 0.0))
                )
                slopes_all[
                    s, rows(me * planes + b, sub), q * columns : (q + 1) * columns
                ] = slope.astype(bf16)
            gaps[b, rows(s, sub), :] = gap

        over(planes, slope_rows)
        for index, (turn, part) in enumerate(own_sends):
            slope_copy(s, me, part, index, peer(turn)).start()

    def relay_slopes(s):
        index = len(own_sends)
        for lead in range(2):
            for turn in across + along:
                part = lead if turn in across else 1 - lead
                source = place_of(peer(turn, -1))
                slope_copy(s, source, part, 0, (role, dp)).wait_recv()
                if lead == 0:
                    for onward in along if turn in across else across:
                        slope_copy(s, source, part, index, peer(onward)).start()
                        index += 1
                for flip in turns:
                    slope_copy(s, source, part, index, peer(flip)).start()
                    index += 1

    def share_corners(s):
        index = slope_sends - 2 * len(corners) * len(turns)
        for turn in corners:
            source = place_of(peer(turn, -1))
            for part in range(2):
                slope_copy(s, source, part, 0, (role, dp)).wait_recv()
                for flip in turns:
                    slope_copy(s, source, part, index, peer(flip)).start()
                    index += 1

    def add_gradient(s):
        for n in range(1, places):
            feature_copy(s, n, True).wait_recv()
            if shifts[n][2]:
                for part in range(2):
                    slope_copy(s, place_of(peer(shifts[n], -1)), part, 0, (role, dp)).wait_recv()

        def book(q):
            out[q] = out[q] + lax.dot_general(
                features_all[s],
                slopes_all[s, :, rows(q, columns)],
                (((0,), (0,)), ((), ())),
                preferred_element_type=f32,
            )

        over(books, book)

    barrier = pltpu.get_barrier_semaphore()

    def greet(step, carry):
        other = lax.rem(plane + step, planes)
        pl.semaphore_signal(barrier, inc=1, device_id=(role, dp, other), device_id_type=MESH)
        return carry

    lax.fori_loop(1, planes, greet, 0)
    for shift in shifts[1:]:
        r, d = peer(shift)
        pl.semaphore_signal(barrier, inc=1, device_id=(r, d, plane), device_id_type=MESH)
    pl.semaphore_wait(barrier, planes - 1 + places - 1)

    def send_labels(step, carry):
        for n in range(2):
            label_copy(n, step, False).start()
        return carry

    lax.fori_loop(1, planes, send_labels, 0)
    for s in range(min(2, rounds)):
        for kind in range(2):
            send_own(kind, s)
    for kind in range(2):
        over(rounds, lambda s: own_local(kind, s).start())
    for kind in range(2):
        over(books, lambda q: weight_copy(kind, q).start())

    targets_all[plane] = targets_in[...]
    segments_all[plane] = segments_in[...]

    def clear(q):
        out[q] = jnp.zeros(out.shape[1:], f32)

    over(books, clear)

    def labels_arrive(step, carry):
        for n in range(2):
            label_copy(n, step, True).wait_recv()
        return carry

    lax.fori_loop(1, planes, labels_arrive, 0)
    length = segments_all.shape[2]
    picks = (
        lax.broadcasted_iota(jnp.int32, (half, length), 1)
        == lax.broadcasted_iota(jnp.int32, (half, length), 0) + role * half
    )

    def unpack(b):
        block = targets_all[b].astype(f32)

        def column(line):
            return jnp.sum(jnp.where(picks, line, 0.0), axis=1, keepdims=True)

        lane = lane_of(half)
        ids = jnp.zeros((half, lanes), jnp.int32)
        for q in range(books):
            ids = jnp.where(lane == q, column(block[q : q + 1, :]).astype(jnp.int32) - plane * columns, ids)
        document = column(segments_all[b].astype(f32))

        def count(p, total):
            same = document == segments_all[p].astype(f32)
            return total + jnp.sum(jnp.where(same, 1.0, 0.0), axis=1, keepdims=True)

        size = lax.fori_loop(0, planes, count, jnp.zeros((half, 1), f32))
        weight = jnp.broadcast_to((planes * length) / ((2 * planes) * size), (half, lanes))
        for s in range(rounds):
            target_lanes[s, rows(b, sub), :] = ids[s * sub : (s + 1) * sub]
            weight_lanes[s, rows(b, sub), :] = weight[s * sub : (s + 1) * sub]

    over(planes, unpack)

    def owns(s):
        for kind in range(2):
            send_own(kind, s)

    def between(low, s, high, also=True):
        return jnp.logical_and(jnp.logical_and(s >= low, s < high), also)

    exchange = remote(swap, both_terms.at[rows(role, half)], swap_sem.at[0], swap_sem.at[1], (1 - role, dp, plane))

    def finish_terms():
        def add_gap(step, total):
            gap_copy(step, True).wait_recv()
            return total + gaps_in[lax.rem(plane + planes - step, planes)]

        gap_total = lax.fori_loop(1, planes, add_gap, gaps[plane])
        student_terms = (
            blend_ratio * sharpness_divisor * sharpness_divisor * gap_total + (1.0 - blend_ratio) * own_terms[1]
        )
        teacher_terms = own_terms[0]
        swap[...] = jnp.where(role == 0, student_terms, teacher_terms)
        both_terms[rows(role, half), :] = jnp.where(role == 0, teacher_terms, student_terms)
        exchange.start()

    @pl.when(middle)
    def _():
        for kind in range(2):
            forward(kind, 0)

    def iteration(s):
        @pl.when(between(1, s, rounds + 1))
        def _():
            compute_slopes(s - 1)

        @pl.when(s == rounds)
        def _():
            def send_gaps(step, carry):
                gap_copy(step, False).start()
                return carry

            lax.fori_loop(1, planes, send_gaps, 0)

        @pl.when(between(0, s, rounds))
        def _():
            teacher_logits(s)

        @pl.when(between(0, s, rounds - 1, middle))
        def _():
            forward(0, s + 1)

        @pl.when(between(0, s, rounds))
        def _():
            student_logits(s)

        @pl.when(between(0, s, rounds - 1, middle))
        def _():
            forward(1, s + 1)

        @pl.when(between(0, s, rounds - 2))
        def _():
            owns(s + 2)

        @pl.when(between(3, s, rounds + 3))
        def _():
            add_gradient(s - 3)

        @pl.when(between(2, s, rounds + 2))
        def _():
            share_corners(s - 2)

        @pl.when(between(1, s, rounds + 1))
        def _():
            relay_slopes(s - 1)

        @pl.when(s == rounds)
        def _():
            finish_terms()

    over(rounds + 3, iteration)

    exchange.wait()
    terms_out[...] = jnp.transpose(both_terms[...])[2 * pitch : 2 * pitch + books]

    def drain_line(step, carry):
        for n in range(2):
            label_copy(n, step, False).wait_send()
        gap_copy(step, False).wait_send()
        over(rounds, lambda s: stats_copy(s, step, False).wait_send())
        return carry

    lax.fori_loop(1, planes, drain_line, 0)

    def drain_round(s):
        for n in range(1, places):
            feature_copy(s, n, False).wait_send()
        for index in range(slope_sends):
            slope_copy(s, me, 0, index, (role, dp)).wait_send()

        def drain_block(b):
            for kind in range(2):

                own = b == plane
                up = jnp.logical_or(passes(b, True), own if skips else jnp.logical_and(own, jnp.logical_not(last)))
                down = jnp.logical_or(passes(b, False), own if skips else jnp.logical_and(own, jnp.logical_not(first)))

                @pl.when(up)
                def _():
                    z_copy(kind, s, b, True, False).wait_send()

                @pl.when(down)
                def _():
                    z_copy(kind, s, b, False, False).wait_send()

        over(planes, drain_block)

    over(rounds, drain_round)


def on_device(
    teacher_states,
    student_states,
    teacher_gain,
    student_gain,
    mentor_output_weights,
    student_heads,
    segments,
    targets,
):
    books, teacher_width, columns = mentor_output_weights.shape
    student_width = student_heads.shape[1]
    roles, dps, planes = (lax.axis_size(name) for name in ("role", "dp", "ctx"))
    inner = 2 if dps % 2 == 0 else 1
    places = roles * dps
    rows_here = teacher_states.shape[1]
    half = rows_here // roles
    rounds = half // sub
    group = planes * sub
    share = student_width // places
    sizes = (roles, dps, planes, inner, books, columns, share, half)

    vmem = pl.BlockSpec(memory_space=pltpu.VMEM)
    hbm = pl.BlockSpec(memory_space=pltpu.HBM)
    dma = pltpu.SemaphoreType.DMA
    shares, terms = pl.pallas_call(
        functools.partial(kernel, sizes),
        out_shape=(
            pltpu.VMEM((books, share, columns), f32),
            jax.ShapeDtypeStruct((books, rows_here), f32),
        ),
        in_specs=[hbm, hbm, vmem, vmem, hbm, hbm, vmem, vmem],
        out_specs=(vmem, vmem),
        scratch_shapes=[
            pltpu.VMEM((rounds, planes, sub, teacher_width), bf16),
            pltpu.VMEM((rounds, planes, sub, student_width), bf16),
            pltpu.VMEM(mentor_output_weights.shape, bf16),
            pltpu.VMEM(student_heads.shape, bf16),
            pltpu.VMEM((group, teacher_width), bf16),
            pltpu.VMEM((group, student_width), bf16),
            pltpu.VMEM((rounds, places, group, share), bf16),
            pltpu.VMEM((rounds, places * group, share), bf16),
            pltpu.VMEM((rounds, places * group, books * columns), bf16),
            pltpu.VMEM((books, group, columns), f32),
            pltpu.VMEM((books, group, columns), f32),
            pltpu.VMEM((planes, books, rows_here), jnp.int32),
            pltpu.VMEM((planes, 1, rows_here), jnp.int32),
            pltpu.VMEM((rounds, group, lanes), jnp.int32),
            pltpu.VMEM((rounds, group, lanes), f32),
            pltpu.VMEM((2 * group, lanes), f32),
            pltpu.VMEM((rounds, planes, 4 * pitch, 2 * group), f32),
            pltpu.VMEM((2 * group, lanes), f32),
            pltpu.VMEM((planes, half, lanes), f32),
            pltpu.VMEM((planes, half, lanes), f32),
            pltpu.VMEM((2, half, lanes), f32),
            pltpu.VMEM((half, lanes), f32),
            pltpu.VMEM((rows_here, lanes), f32),
            dma((2, 2, rounds, planes)),
            dma((2, rounds, planes)),
            dma((2, rounds)),
            dma((2, books)),
            dma((2, planes)),
            dma((2, planes)),
            dma((rounds, planes)),
            dma((rounds, planes)),
            dma((rounds, places)),
            dma((rounds, places)),
            dma((rounds, 4 * places)),
            dma((rounds, places, 2)),
            dma((planes,)),
            dma((planes,)),
            dma((2,)),
        ],
        compiler_params=pltpu.CompilerParams(
            collective_id=0, has_side_effects=True, vmem_limit_bytes=67_043_328 - 4 * books * share * columns - (1 << 17)
        ),
        name="distill",
    )(
        teacher_states[0],
        student_states[0],
        teacher_gain.reshape(-1, lanes),
        student_gain.reshape(-1, lanes),
        mentor_output_weights,
        student_heads,
        targets[0].T,
        segments,
    )
    return shares, terms.T.reshape(1, 1, rows_here, books)


def solution(mesh):
    return jax.shard_map(
        on_device,
        mesh=mesh,
        in_specs=(
            P("dp", "ctx", None),
            P("dp", "ctx", None),
            P(),
            P(),
            P(None, None, "ctx"),
            P(None, None, "ctx"),
            P("dp", "ctx"),
            P("dp", "ctx", None),
        ),
        out_specs=(P(None, ("role", "dp"), "ctx"), P("role", "dp", "ctx", None)),
        check_vma=False,
    )
```
